8 devices in a mesh: tp: 2 (over z, y), ep: 4 (over x, core).
Axes of the slice: x: 2, y: 2, z: 1, core: 2. Of those that a mesh axis runs over, the one named last changes fastest.
Arguments:
- x_tok: bfloat16 [32768, 768], P('ep')
- dy_tok: bfloat16 [32768, 768], P('ep')
- route_idx: int32 [32768, 2], P('ep')
- norm_scale: float32 [768], replicated
- w_router: float32 [768, 32], replicated
- w_gate: bfloat16 [32, 768, 3072], P('ep', None, 'tp')
- w_lin: bfloat16 [32, 768, 3072], P('ep', None, 'tp')
- w_out: bfloat16 [32, 3072, 768], P('ep', 'tp')
Outputs:
- output 1: bfloat16 [32768, 768], P('ep')
- output 2: float32 [2], replicated
- output 3: bfloat16 [32768, 768], P('ep')
- output 4: float32 [768], replicated
- output 5: float32 [768, 32], replicated
- output 6: float32 [32, 768, 3072], P('ep', None, 'tp')
- output 7: float32 [32, 768, 3072], P('ep', None, 'tp')
- output 8: float32 [32, 3072, 768], P('ep', 'tp')
All inputs are finite; a program needn't handle non-finite values.
Results may differ from the reference program's by a relative error of at most 0.015982.
Values are sent between devices in bfloat16 or wider.
A program may use at most 1 GiB of HBM per device.

```python
import jax
import jax.numpy as jnp
from jax import lax

MODEL_DIM = 768
FF_DIM = 3072
EXPERTS = 32
TOK_DEV = 8192
GROUPS = 4
TOKENS = TOK_DEV * GROUPS
SLOT_CAP = (5 * TOK_DEV + 2 * EXPERTS - 1) // (2 * EXPERTS)
NORM_EPS = 1e-6
Z_COEF = 0.001
AUX_COEF = 0.01


def draw_routes(root_key, tok_count, expert_count):
    sub_keys = jax.random.split(root_key, 4)
    expert_order = jax.random.permutation(sub_keys[0], expert_count)
    pick_left = jax.random.randint(sub_keys[1], (tok_count,), 0, expert_count)
    pick_right = jax.random.randint(sub_keys[2], (tok_count,), 0, expert_count)
    first_ids = expert_order[jnp.minimum(pick_left, pick_right)]
    step_size = jax.random.randint(sub_keys[3], (tok_count,), 1, expert_count)
    second_ids = (first_ids + step_size) % expert_count
    return jnp.stack([first_ids, second_ids], axis=1).astype(jnp.int32)


def setup_inputs(seed: int = 0) -> dict:
    sub_keys = jax.random.split(jax.random.key(seed), 8)
    x_tok = jax.random.normal(sub_keys[0], (TOKENS, MODEL_DIM), jnp.float32).astype(jnp.bfloat16)
    dy_tok = (jax.random.normal(sub_keys[1], (TOKENS, MODEL_DIM), jnp.float32) * MODEL_DIM ** -0.5).astype(jnp.bfloat16)
    route_idx = draw_routes(sub_keys[2], TOKENS, EXPERTS)
    norm_scale = 1.0 + 0.3 * jax.random.normal(sub_keys[3], (MODEL_DIM,), jnp.float32)
    w_router = jax.random.normal(sub_keys[4], (MODEL_DIM, EXPERTS), jnp.float32) * (4.0 * MODEL_DIM ** -0.5)
    w_gate = (jax.random.normal(sub_keys[5], (EXPERTS, MODEL_DIM, FF_DIM), jnp.float32) * MODEL_DIM ** -0.5).astype(jnp.bfloat16)
    w_lin = (jax.random.normal(sub_keys[6], (EXPERTS, MODEL_DIM, FF_DIM), jnp.float32) * MODEL_DIM ** -0.5).astype(jnp.bfloat16)
    w_out = (jax.random.normal(sub_keys[7], (EXPERTS, FF_DIM, MODEL_DIM), jnp.float32) * (1.5 * FF_DIM ** -0.5)).astype(jnp.bfloat16)
    return {'x_tok': x_tok, 'dy_tok': dy_tok, 'route_idx': route_idx, 'norm_scale': norm_scale, 'w_router': w_router, 'w_gate': w_gate, 'w_lin': w_lin, 'w_out': w_out}


def gelu_fn(pre_act):
    return jax.nn.gelu(pre_act, approximate=True)


def route_slots(route_ids, experts, slot_cap, stride):
    expert_ids = jnp.arange(experts, dtype=jnp.int32)
    hit_first = (route_ids[:, 0:1] == expert_ids).astype(jnp.int32)
    hit_second = (route_ids[:, 1:2] == expert_ids).astype(jnp.int32)
    rank_first = jnp.cumsum(hit_first, axis=0) - hit_first
    rank_second = jnp.cumsum(hit_second, axis=0) - hit_second + jnp.sum(hit_first, axis=0)
    pos_first = jnp.sum(rank_first * hit_first, axis=1)
    pos_second = jnp.sum(rank_second * hit_second, axis=1)
    overflow = experts * stride
    slot_first = jnp.where(pos_first < slot_cap, route_ids[:, 0] * stride + pos_first, overflow)
    slot_second = jnp.where(pos_second < slot_cap, route_ids[:, 1] * stride + pos_second, overflow)
    return slot_first, slot_second


def slot_tables(slot_first, slot_second, gate_first, gate_second, slot_total):
    tok_count = slot_first.shape[0]
    tok_ids = jnp.arange(tok_count, dtype=jnp.int32)
    slot_tok = jnp.full((slot_total + 1,), tok_count, jnp.int32)
    slot_tok = slot_tok.at[slot_first].set(tok_ids).at[slot_second].set(tok_ids)
    slot_gate = jnp.zeros((slot_total + 1,), jnp.float32)
    slot_gate = slot_gate.at[slot_first].set(gate_first).at[slot_second].set(gate_second)
    return slot_tok[:slot_total], slot_gate[:slot_total]


def pick_rows(row_data, slot_index):
    return jnp.take(row_data, slot_index, axis=0, mode='fill', fill_value=0)


def reference(x_tok, dy_tok, route_idx, norm_scale, w_router, w_gate, w_lin, w_out):
    x_wide = x_tok.astype(jnp.float32)
    inv_rms = lax.rsqrt(jnp.mean(x_wide * x_wide, axis=-1, keepdims=True) + NORM_EPS)
    x_norm = x_wide * inv_rms
    u_tok = (x_norm * norm_scale).astype(jnp.bfloat16)
    u_wide = u_tok.astype(jnp.float32)
    logits = jnp.dot(u_wide, w_router, preferred_element_type=jnp.float32)
    log_norm = jax.nn.logsumexp(logits, axis=-1)
    router_prob = jnp.exp(logits - log_norm[:, None])
    expert_ids = jnp.arange(EXPERTS, dtype=jnp.int32)
    one_first = (route_idx[:, 0:1] == expert_ids).astype(jnp.float32)
    one_second = (route_idx[:, 1:2] == expert_ids).astype(jnp.float32)
    frac_first = jnp.sum(one_first, axis=0) / TOKENS
    mean_prob = jnp.sum(router_prob, axis=0) / TOKENS
    z_loss = Z_COEF * jnp.sum(log_norm * log_norm) / TOKENS
    aux_loss = AUX_COEF * EXPERTS * jnp.sum(frac_first * mean_prob)
    gate_first = jnp.sum(router_prob * one_first, axis=-1)
    gate_second = jnp.sum(router_prob * one_second, axis=-1)
    gate_total = gate_first + gate_second
    norm_first = gate_first / gate_total
    norm_second = gate_second / gate_total
    gate_wide = w_gate.astype(jnp.float32)
    lin_wide = w_lin.astype(jnp.float32)
    out_wide = w_out.astype(jnp.float32)

    def group_step(grad_acc, group_in):
        ids_grp, u_grp, dy_grp, first_grp, second_grp = group_in
        slot_first, slot_second = route_slots(ids_grp, EXPERTS, SLOT_CAP, SLOT_CAP)
        slot_tok, slot_gate = slot_tables(slot_first, slot_second, first_grp, second_grp, EXPERTS * SLOT_CAP)
        disp_rows = pick_rows(u_grp, slot_tok).reshape(EXPERTS, SLOT_CAP, MODEL_DIM).astype(jnp.float32)
        a_gate = jnp.einsum('ecd,edf->ecf', disp_rows, gate_wide)
        a_lin = jnp.einsum('ecd,edf->ecf', disp_rows, lin_wide)
        gelu_val, gelu_back = jax.vjp(gelu_fn, a_gate)
        hidden = (gelu_val * a_lin).astype(jnp.bfloat16).astype(jnp.float32)
        exp_out = jnp.einsum('ecf,efd->ecd', hidden, out_wide).astype(jnp.bfloat16)
        exp_out = exp_out.reshape(EXPERTS * SLOT_CAP, MODEL_DIM)
        out_first = pick_rows(exp_out, slot_first)
        out_second = pick_rows(exp_out, slot_second)
        do_slot = (pick_rows(dy_grp, slot_tok).astype(jnp.float32) * slot_gate[:, None]).astype(jnp.bfloat16)
        do_slot = do_slot.astype(jnp.float32).reshape(EXPERTS, SLOT_CAP, MODEL_DIM)
        d_hidden = jnp.einsum('ecd,efd->ecf', do_slot, out_wide)
        da_gate = gelu_back(d_hidden * a_lin)[0].astype(jnp.bfloat16).astype(jnp.float32)
        da_lin = (d_hidden * gelu_val).astype(jnp.bfloat16).astype(jnp.float32)
        du_slot = jnp.einsum('ecf,edf->ecd', da_gate, gate_wide) + jnp.einsum('ecf,edf->ecd', da_lin, lin_wide)
        du_slot = du_slot.astype(jnp.bfloat16).reshape(EXPERTS * SLOT_CAP, MODEL_DIM)
        du_exp = pick_rows(du_slot, slot_first).astype(jnp.float32) + pick_rows(du_slot, slot_second).astype(jnp.float32)
        acc_gate, acc_lin, acc_out = grad_acc
        acc_gate = acc_gate + jnp.einsum('ecd,ecf->edf', disp_rows, da_gate)
        acc_lin = acc_lin + jnp.einsum('ecd,ecf->edf', disp_rows, da_lin)
        acc_out = acc_out + jnp.einsum('ecf,ecd->efd', hidden, do_slot)
        return (acc_gate, acc_lin, acc_out), (out_first, out_second, du_exp)

    group_in = (route_idx.reshape(GROUPS, TOK_DEV, 2), u_tok.reshape(GROUPS, TOK_DEV, MODEL_DIM), dy_tok.reshape(GROUPS, TOK_DEV, MODEL_DIM), norm_first.reshape(GROUPS, TOK_DEV), norm_second.reshape(GROUPS, TOK_DEV))
    grad_init = (jnp.zeros((EXPERTS, MODEL_DIM, FF_DIM), jnp.float32), jnp.zeros((EXPERTS, MODEL_DIM, FF_DIM), jnp.float32), jnp.zeros((EXPERTS, FF_DIM, MODEL_DIM), jnp.float32))
    grad_sums, per_group = lax.scan(group_step, grad_init, group_in)
    d_gate, d_lin, d_out = grad_sums
    out_first = per_group[0].reshape(TOKENS, MODEL_DIM).astype(jnp.float32)
    out_second = per_group[1].reshape(TOKENS, MODEL_DIM).astype(jnp.float32)
    du_exp = per_group[2].reshape(TOKENS, MODEL_DIM)
    y_tok = (x_wide + norm_first[:, None] * out_first + norm_second[:, None] * out_second).astype(jnp.bfloat16)
    dy_wide = dy_tok.astype(jnp.float32)
    dn_first = jnp.sum(dy_wide * out_first, axis=-1)
    dn_second = jnp.sum(dy_wide * out_second, axis=-1)
    gate_mix = norm_first * dn_first + norm_second * dn_second
    aux_coef = AUX_COEF * EXPERTS * frac_first
    d_logits = router_prob * (aux_coef - jnp.sum(aux_coef * router_prob, axis=-1, keepdims=True))
    d_logits = d_logits + (2.0 * Z_COEF) * log_norm[:, None] * router_prob
    d_logits = d_logits + one_first * (norm_first * (dn_first - gate_mix))[:, None]
    d_logits = d_logits + one_second * (norm_second * (dn_second - gate_mix))[:, None]
    d_router = jnp.dot(u_wide.T, d_logits, preferred_element_type=jnp.float32)
    du_all = du_exp + jnp.dot(d_logits, w_router.T, preferred_element_type=jnp.float32)
    d_scale = jnp.sum(du_all * x_norm, axis=0)
    dx_norm = du_all * norm_scale
    dx_tok = (dy_wide + inv_rms * (dx_norm - x_norm * jnp.mean(dx_norm * x_norm, axis=-1, keepdims=True))).astype(jnp.bfloat16)
    losses = jnp.stack([z_loss, aux_loss])
    return (y_tok, losses, dx_tok, d_scale, d_router, d_gate, d_lin, d_out)
```

```python
import functools

import jax
import jax.numpy as jnp
from jax import lax
from jax.experimental import pallas as pl
from jax.experimental.pallas import tpu as pltpu
from jax.sharding import PartitionSpec as P


NORM_EPS = 1e-6
Z_COEF = 0.001
AUX_COEF = 0.01
GELU_A = 0.7978845608028654
GELU_B = 0.044715


def ffn_kernel(tp_ref, x_ref, dy_ref, gate_ref, scale_ref, wg_ref, wl_ref, wo_ref, *refs):
    (u_out, do_out, h_out, da_out, db_out, ok_out, os_out, dk_out, ds_out, u_s, do_s, o_acc, du_acc) = refs[-13:]
    f_id = pl.program_id(1)
    half = ok_out.shape[-1]

    @pl.when(f_id == 0)
    def _():
        gate = gate_ref[0]
        live = jnp.logical_not(gate < 0.0)
        x_wide = x_ref[0].astype(jnp.float32)
        inv = lax.rsqrt(jnp.mean(x_wide * x_wide, axis=-1, keepdims=True) + NORM_EPS)
        u_val = jnp.where(live, (x_wide * inv) * scale_ref[...], 0.0).astype(jnp.bfloat16)
        do_val = jnp.where(live, dy_ref[0].astype(jnp.float32) * gate, 0.0).astype(jnp.bfloat16)
        u_s[...] = u_val
        do_s[...] = do_val
        u_out[0, 0] = u_val
        do_out[0, 0] = do_val

    u_val = u_s[...]
    do_val = do_s[...]
    wg = wg_ref[0]
    wl = wl_ref[0]
    wo = wo_ref[0]
    nn = (((1,), (0,)), ((), ()))
    nt = (((1,), (1,)), ((), ()))
    dot = functools.partial(lax.dot_general, preferred_element_type=jnp.float32)
    a0 = dot(u_val, wg, nn)
    a1 = dot(u_val, wl, nn)
    dh = dot(do_val, wo, nt)
    sq = a0 * a0
    th = jnp.tanh(GELU_A * (a0 + GELU_B * (a0 * sq)))
    cdf = 0.5 + 0.5 * th
    ge = a0 * cdf
    slope = cdf + 0.5 * a0 * ((1.0 - th * th) * (GELU_A + (3.0 * GELU_A * GELU_B) * sq))
    h_val = (ge * a1).astype(jnp.bfloat16)
    da = (dh * a1 * slope).astype(jnp.bfloat16)
    db = (dh * ge).astype(jnp.bfloat16)
    h_out[0, 0] = h_val
    da_out[0, 0] = da
    db_out[0, 0] = db
    o_new = dot(h_val, wo, nn)
    du_new = dot(da, wg, nt) + dot(db, wl, nt)

    o_acc[...] = jnp.where(f_id == 0, 0.0, o_acc[...]) + o_new
    du_acc[...] = jnp.where(f_id == 0, 0.0, du_acc[...]) + du_new

    @pl.when(f_id == pl.num_programs(1) - 1)
    def _():
        first = tp_ref[0] == 0
        for acc, keep, send in ((o_acc, ok_out, os_out), (du_acc, dk_out, ds_out)):
            low = acc[:, :half].astype(jnp.bfloat16)
            high = acc[:, half:].astype(jnp.bfloat16)
            keep[0] = jnp.where(first, low, high)
            send[0] = jnp.where(first, high, low)


def router_kernel(blocks, cap, experts, local_exp, ep_ref, x_ref, idx_ref, scale_ref, wr_ref, prob_ref, col_ref, row_ref, tab_ref, sum_ref, carry, prob_acc, sq_acc):
    step = pl.program_id(0)
    rows = x_ref.shape[0]
    first = idx_ref[:, 0:1]
    second = idx_ref[:, 1:2]
    pair_lane = lax.broadcasted_iota(jnp.int32, (rows, 2 * experts), 1)

    @pl.when(step == 0)
    def _():
        carry[...] = jnp.zeros_like(carry)
        prob_acc[...] = jnp.zeros_like(prob_acc)
        sq_acc[...] = jnp.zeros_like(sq_acc)
        tab_ref[...] = jnp.zeros_like(tab_ref)

    @pl.when(step < blocks)
    def _():
        carry[...] += jnp.sum(jnp.where(first + experts == pair_lane, 1.0, 0.0), axis=0, keepdims=True)

    @pl.when(step >= blocks)
    def _():
        x_wide = x_ref[...].astype(jnp.float32)
        inv = lax.rsqrt(jnp.mean(x_wide * x_wide, axis=-1, keepdims=True) + NORM_EPS)
        u_val = ((x_wide * inv) * scale_ref[...]).astype(jnp.bfloat16)
        logits = jnp.dot(u_val.astype(jnp.float32), wr_ref[...], preferred_element_type=jnp.float32)
        top = jnp.max(logits, axis=-1, keepdims=True)
        log_norm = top + jnp.log(jnp.sum(jnp.exp(logits - top), axis=-1, keepdims=True))
        prob = jnp.exp(logits - log_norm)
        prob_ref[...] = prob
        prob_acc[...] += jnp.sum(prob, axis=0, keepdims=True)
        sq_acc[...] += jnp.sum(log_norm * log_norm, axis=0, keepdims=True)
        lane = lax.broadcasted_iota(jnp.int32, (rows, experts), 1)
        p_first = jnp.sum(jnp.where(first == lane, prob, 0.0), axis=-1, keepdims=True)
        p_second = jnp.sum(jnp.where(second == lane, prob, 0.0), axis=-1, keepdims=True)
        total = p_first + p_second
        n_first = p_first / total
        n_second = p_second / total
        sel_first = first == pair_lane
        sel_second = second + experts == pair_lane
        hits = jnp.where(sel_first | sel_second, 1.0, 0.0)
        below = lax.broadcasted_iota(jnp.int32, (rows, rows), 1) < lax.broadcasted_iota(jnp.int32, (rows, rows), 0)
        ranks = jnp.dot(jnp.where(below, 1.0, 0.0).astype(jnp.bfloat16), hits.astype(jnp.bfloat16), preferred_element_type=jnp.float32) + carry[...]
        carry[...] += jnp.sum(hits, axis=0, keepdims=True)
        pos_first = jnp.sum(jnp.where(sel_first, ranks, 0.0), axis=-1, keepdims=True).astype(jnp.int32)
        pos_second = jnp.sum(jnp.where(sel_second, ranks, 0.0), axis=-1, keepdims=True).astype(jnp.int32)
        for c, (route, pos) in enumerate(((first, pos_first), (second, pos_second))):
            kept = pos < cap
            owner = route // local_exp
            spot = (owner ^ ep_ref[0]) * (local_exp * cap) + (route - owner * local_exp) * cap + pos
            row_ref[:, c:c + 1] = jnp.where(kept, spot, 0)
            col_ref[:, 2 + c:3 + c] = jnp.where(kept, 1.0, 0.0)
        col_ref[:, 0:1] = n_first
        col_ref[:, 1:2] = n_second
        col_ref[:, 4:5] = inv
        col_ref[:, 5:6] = log_norm
        col_ref[:, 6:8] = jnp.zeros((rows, 2), jnp.float32)
        token = lax.broadcasted_iota(jnp.int32, (rows, 1), 0) + ((step - blocks) * rows + 1)
        tok_hi = (token // 128).astype(jnp.float32)
        tok_lo = (token % 128).astype(jnp.float32)
        wide = lax.broadcasted_iota(jnp.int32, (rows, 5 * experts), 1)
        expert = wide % experts
        place = lax.broadcasted_iota(jnp.int32, (rows, cap), 1)
        for route, pos, gate in ((first, pos_first, n_first), (second, pos_second, n_second)):
            hi = gate.astype(jnp.bfloat16).astype(jnp.float32)
            rest = gate - hi
            mid = rest.astype(jnp.bfloat16).astype(jnp.float32)
            vals = jnp.where(wide < experts, tok_hi, jnp.where(wide < 2 * experts, tok_lo, jnp.where(wide < 3 * experts, hi, jnp.where(wide < 4 * experts, mid, rest - mid))))
            left = jnp.where(expert == route, vals, 0.0).astype(jnp.bfloat16)
            right = jnp.where(place == pos, 1.0, 0.0).astype(jnp.bfloat16)
            tab_ref[...] += lax.dot_general(left, right, (((0,), (0,)), ((), ())), preferred_element_type=jnp.float32)

    @pl.when(step == 2 * blocks - 1)
    def _():
        sum_ref[...] = jnp.zeros_like(sum_ref)
        sum_ref[0:1, 0:experts] = carry[:, :experts]
        sum_ref[1:2, 0:experts] = prob_acc[...]
        sum_ref[2:3, 0:1] = sq_acc[...]


def router_call(ep_vec, x_loc, idx_loc, scale_row, w_router, cap, local_exp, block):
    rows, width = x_loc.shape
    experts = w_router.shape[1]
    blocks = rows // block

    def late(i, ep):
        return jnp.maximum(i - blocks, 0), 0

    def fixed(i, ep):
        return 0, 0

    return pl.pallas_call(
        functools.partial(router_kernel, blocks, cap, experts, local_exp),
        grid_spec=pltpu.PrefetchScalarGridSpec(
            num_scalar_prefetch=1,
            grid=(2 * blocks,),
            in_specs=[
                pl.BlockSpec((block, width), late),
                pl.BlockSpec((block, 2), lambda i, ep: (jnp.where(i < blocks, i, i - blocks), 0)),
                pl.BlockSpec((1, width), fixed),
                pl.BlockSpec((width, experts), fixed),
            ],
            out_specs=[pl.BlockSpec((block, experts), late), pl.BlockSpec((block, 8), late), pl.BlockSpec((block, 2), late), pl.BlockSpec((5 * experts, cap), fixed), pl.BlockSpec((8, 128), fixed)],
            scratch_shapes=[pltpu.VMEM((1, 2 * experts), jnp.float32), pltpu.VMEM((1, experts), jnp.float32), pltpu.VMEM((1, 1), jnp.float32)],
        ),
        out_shape=[
            jax.ShapeDtypeStruct((rows, experts), jnp.float32),
            jax.ShapeDtypeStruct((rows, 8), jnp.float32),
            jax.ShapeDtypeStruct((rows, 2), jnp.int32),
            jax.ShapeDtypeStruct((5 * experts, cap), jnp.float32),
            jax.ShapeDtypeStruct((8, 128), jnp.float32),
        ],
        compiler_params=pltpu.CompilerParams(dimension_semantics=("arbitrary",)),
        cost_estimate=pl.CostEstimate(flops=10_000_000_000, bytes_accessed=4 * rows * width, transcendentals=0),
        name="router",
    )(ep_vec, x_loc, idx_loc, scale_row, w_router)


def gather_kernel(parts, fills, blk, rows, group, cols, idx_ref, *refs):
    srcs, out_ref, store, stage = refs[:parts], refs[parts], refs[parts + 1], refs[parts + 2]
    step = pl.program_id(0)
    for p in range(parts):

        @pl.when((step >= p * fills) & (step < (p + 1) * fills))
        def _(p=p):
            val = srcs[p][...].astype(jnp.float32)
            base = pl.multiple_of(step * (blk * 8), blk * 8)
            for j in range(cols):
                store[pl.ds(base + j, blk, stride=8), :] = val[:, j * 128:(j + 1) * 128]

    @pl.when(step >= parts * fills)
    def _():
        start = (step - parts * fills) * rows

        def body(q, carry):
            base = q * group
            vals = [store[pl.ds(pl.multiple_of(idx_ref[start + base + r] * 8, 8), 8), :] for r in range(group)]
            for r in range(group):
                stage[pl.ds(pl.multiple_of((base + r) * 8, 8), 8), :] = vals[r]
            return carry

        lax.fori_loop(0, rows // group, body, 0)
        for j in range(cols):
            out_ref[:, j * 128:(j + 1) * 128] = stage[pl.ds(j, rows, stride=8), :].astype(out_ref.dtype)


def gather_rows(srcs, idx, blk, rows, group):
    parts = len(srcs)
    count, width = srcs[0].shape
    fills = count // blk
    total = parts * fills

    def src_map(p, i):
        return jnp.clip(i - p * fills, 0, fills - 1), 0

    return pl.pallas_call(
        functools.partial(gather_kernel, parts, fills, blk, rows, group, width // 128),
        grid=(total + idx.shape[0] // rows,),
        in_specs=[pl.BlockSpec(memory_space=pltpu.SMEM)] + [pl.BlockSpec((blk, width), functools.partial(src_map, p)) for p in range(parts)],
        out_specs=pl.BlockSpec((rows, width), lambda i: (jnp.maximum(i - total, 0), 0)),
        out_shape=jax.ShapeDtypeStruct((idx.shape[0], width), jnp.bfloat16),
        scratch_shapes=[pltpu.VMEM((parts * count * 8, 128), jnp.float32), pltpu.VMEM((rows * 8, 128), jnp.float32)],
        compiler_params=pltpu.CompilerParams(dimension_semantics=("arbitrary",), vmem_limit_bytes=60 * 1024 * 1024),
        cost_estimate=pl.CostEstimate(flops=40_000_000_000, bytes_accessed=4 * width * idx.shape[0], transcendentals=0),
        name="gather_rows",
    )(idx, *srcs)


def combine_kernel(tp_ref, x_ref, dy_ref, o1_ref, o2_ref, col_ref, y_ref, dn_ref):
    col = col_ref[...]
    o1 = jnp.where(col[:, 2:3] > 0.0, o1_ref[...].astype(jnp.float32), 0.0)
    o2 = jnp.where(col[:, 3:4] > 0.0, o2_ref[...].astype(jnp.float32), 0.0)
    y_ref[...] = (x_ref[...].astype(jnp.float32) + col[:, 0:1] * o1 + col[:, 1:2] * o2).astype(y_ref.dtype)
    dy = dy_ref[...].astype(jnp.float32)
    dn_ref[:, 0:1] = jnp.sum(dy * o1, axis=-1, keepdims=True)
    dn_ref[:, 1:2] = jnp.sum(dy * o2, axis=-1, keepdims=True)


def norm_kernel(tp_ref, x_ref, d1_ref, d2_ref, prob_ref, idx_ref, dn_ref, aux_ref, wr_ref, scale_ref, col_ref, dxn_ref, mix_ref, ds_ref, dr_ref):
    col = col_ref[...]
    n_first, n_second = col[:, 0:1], col[:, 1:2]
    dn_first, dn_second = dn_ref[:, 0:1], dn_ref[:, 1:2]
    prob = prob_ref[...]
    aux = aux_ref[...]
    lane = lax.broadcasted_iota(jnp.int32, prob.shape, 1)
    gate_mix = n_first * dn_first + n_second * dn_second
    dl = prob * (aux - jnp.sum(aux * prob, axis=-1, keepdims=True))
    dl = dl + (2.0 * Z_COEF) * col[:, 5:6] * prob
    dl = dl + jnp.where(idx_ref[:, 0:1] == lane, n_first * (dn_first - gate_mix), 0.0)
    dl = dl + jnp.where(idx_ref[:, 1:2] == lane, n_second * (dn_second - gate_mix), 0.0)
    du = jnp.where(col[:, 2:3] > 0.0, d1_ref[...].astype(jnp.float32), 0.0) + jnp.where(col[:, 3:4] > 0.0, d2_ref[...].astype(jnp.float32), 0.0)
    du = du + lax.dot_general(dl, wr_ref[...], (((1,), (1,)), ((), ())), preferred_element_type=jnp.float32)
    xn = x_ref[...].astype(jnp.float32) * col[:, 4:5]
    dxn = du * scale_ref[...]
    dxn_ref[...] = dxn
    mix_ref[...] = jnp.sum(dxn * xn, axis=-1, keepdims=True)
    u_wide = (xn * scale_ref[...]).astype(jnp.bfloat16).astype(jnp.float32)
    ds = jnp.sum(du * xn, axis=0, keepdims=True)
    dr = lax.dot_general(u_wide, dl, (((0,), (0,)), ((), ())), preferred_element_type=jnp.float32)

    @pl.when(pl.program_id(0) == 0)
    def _():
        ds_ref[...] = ds
        dr_ref[...] = dr

    @pl.when(pl.program_id(0) > 0)
    def _():
        ds_ref[...] += ds
        dr_ref[...] += dr


def dx_kernel(tp_ref, x_ref, dy_ref, dxn_ref, col_ref, mix_ref, dx_ref):
    inv = col_ref[:, 4:5]
    xn = x_ref[...].astype(jnp.float32) * inv
    dx_ref[...] = (dy_ref[...].astype(jnp.float32) + inv * (dxn_ref[...] - xn * mix_ref[...])).astype(dx_ref.dtype)


def join_kernel(tp_ref, own_ref, other_ref, out_ref):
    half = own_ref.shape[1]
    own, other = own_ref[...], other_ref[...]
    first = tp_ref[0] == 0
    out_ref[:, :half] = jnp.where(first, own, other)
    out_ref[:, half:] = jnp.where(first, other, own)


def rows_call(kernel, tp_vec, ins, outs, rows, block):
    specs, args = [], []
    for kind, arr in ins:
        if kind == 'half':
            specs.append(pl.BlockSpec((block, arr.shape[1] // 2), lambda i, tp: (i, tp[0])))
        elif kind == 'row':
            specs.append(pl.BlockSpec((block, arr.shape[1]), lambda i, tp: (i, 0)))
        elif kind == 'same':
            specs.append(pl.BlockSpec(arr.shape, lambda i, tp: (0, 0)))
        elif kind == 'lanes':
            specs.append(pl.BlockSpec((1, arr.shape[1] // 2), lambda i, tp: (0, tp[0])))
        else:
            specs.append(pl.BlockSpec((arr.shape[0] // 2, arr.shape[1]), lambda i, tp: (tp[0], 0)))
        args.append(arr)
    out_specs = [pl.BlockSpec((block if o.shape[0] == rows else o.shape[0], o.shape[1]), (lambda i, tp: (i, 0)) if o.shape[0] == rows else (lambda i, tp: (0, 0))) for o in outs]
    return pl.pallas_call(
        kernel,
        grid_spec=pltpu.PrefetchScalarGridSpec(num_scalar_prefetch=1, grid=(rows // block,), in_specs=specs, out_specs=out_specs),
        out_shape=outs,
        compiler_params=pltpu.CompilerParams(dimension_semantics=("arbitrary",)),
        cost_estimate=pl.CostEstimate(flops=10_000_000_000, bytes_accessed=sum(a.size * 2 for _, a in ins), transcendentals=0),
    )(tp_vec, *args)


def ffn_call(k, base, count, chunks, tp_id, x_rows, dy_rows, gate, scale, wg, wl, wo, bufs, tile):
    experts, rows, width = x_rows.shape
    ff = wg.shape[2]
    steps = ff // tile
    half = width // 2
    row_spec = pl.BlockSpec((1, rows, width), lambda e, f: (base + e, 0, 0))
    in_specs = [
        pl.BlockSpec(memory_space=pltpu.SMEM),
        row_spec,
        row_spec,
        pl.BlockSpec((1, rows, 1), lambda e, f: (base + e, 0, 0)),
        pl.BlockSpec((1, width), lambda e, f: (0, 0)),
        pl.BlockSpec((1, width, tile), lambda e, f: (base + e, 0, f)),
        pl.BlockSpec((1, width, tile), lambda e, f: (base + e, 0, f)),
        pl.BlockSpec((1, tile, width), lambda e, f: (base + e, f, 0)),
    ]
    wide_spec = pl.BlockSpec((1, 1, rows, width), lambda e, f: (k, base + e, 0, 0))
    tile_spec = pl.BlockSpec((1, 1, rows, tile), lambda e, f: (k, base + e, 0, f))
    half_spec = pl.BlockSpec((1, rows, half), lambda e, f: (e, 0, 0))
    wide = jax.ShapeDtypeStruct((chunks, experts, rows, width), jnp.bfloat16)
    deep = jax.ShapeDtypeStruct((chunks, experts, rows, ff), jnp.bfloat16)
    part = jax.ShapeDtypeStruct((count, rows, half), jnp.bfloat16)
    aliases = {}
    if bufs is None:
        bufs = ()
    else:
        aliases = {len(in_specs) + i: i for i in range(5)}
    in_specs = in_specs + [pl.BlockSpec(memory_space=pl.ANY)] * len(bufs)
    flops = 12 * count * rows * width * ff
    outs = pl.pallas_call(
        ffn_kernel,
        grid=(count, steps),
        in_specs=in_specs,
        out_specs=[wide_spec, wide_spec, tile_spec, tile_spec, tile_spec, half_spec, half_spec, half_spec, half_spec],
        out_shape=[wide, wide, deep, deep, deep, part, part, part, part],
        scratch_shapes=[
            pltpu.VMEM((rows, width), jnp.bfloat16),
            pltpu.VMEM((rows, width), jnp.bfloat16),
            pltpu.VMEM((rows, width), jnp.float32),
            pltpu.VMEM((rows, width), jnp.float32),
        ],
        input_output_aliases=aliases,
        compiler_params=pltpu.CompilerParams(dimension_semantics=("arbitrary", "arbitrary"), vmem_limit_bytes=48 * 1024 * 1024),
        cost_estimate=pl.CostEstimate(flops=flops, bytes_accessed=8 * count * rows * (width + ff), transcendentals=count * rows * ff),
        name="ffn",
    )(tp_id, x_rows, dy_rows, gate, scale, wg, wl, wo, *bufs)
    return tuple(outs[:5]), outs[5:]


def solution(mesh):
    ep_size = mesh.shape['ep']

    def swap(arr, k):
        return lax.ppermute(arr, 'ep', [(i, i ^ k) for i in range(ep_size)])

    def swap_tp(arr):
        return lax.ppermute(arr, 'tp', [(0, 1), (1, 0)])

    def device_body(x_loc, dy_loc, idx_loc, norm_scale, w_router, gate_loc, lin_loc, out_loc):
        tok_count, width = x_loc.shape
        experts = w_router.shape[1]
        local_exp = gate_loc.shape[0]
        half = width // 2
        tokens = tok_count * ep_size
        cap = (5 * tok_count + 2 * experts - 1) // (2 * experts)
        ep_id = lax.axis_index('ep')
        tp_id = lax.axis_index('tp')
        tp_vec = tp_id.reshape(1).astype(jnp.int32)
        part_rows = tok_count // 2
        x_near = swap(lax.dynamic_slice_in_dim(x_loc, tp_id * part_rows, part_rows, 0), 2)
        dy_far = swap(dy_loc, 2)
        x_side = swap_tp(x_near)
        x_rows = [[x_loc], [swap(x_loc, 1)], [x_near, x_side], [swap(x_near, 1), swap(x_side, 1)]]
        dy_rows = [[dy_loc], [swap(dy_loc, 1)], [dy_far], [swap(dy_far, 1)]]
        scale_row = norm_scale.reshape(1, width)
        prob, cols, rows, tab, sums_own = router_call(ep_id.reshape(1).astype(jnp.int32), x_loc, idx_loc, scale_row, w_router, cap, local_exp, 512)
        tab = tab.reshape(5, experts, cap)
        slot_one = tab[0] * 128.0 + tab[1]
        slot_gate = jnp.where(slot_one > 0.0, (tab[2] + tab[3]) + tab[4], -1.0)
        pair = jnp.stack([slot_one, slot_gate], axis=1).reshape(ep_size, local_exp, 2, cap)
        sums_far = [swap(sums_own, k) for k in range(1, ep_size)]
        bufs = None
        tables = [lax.dynamic_index_in_dim(pair, ep_id ^ k, 0, keepdims=False) for k in range(ep_size)]
        tables = [swap(tables[k], k) if k else tables[k] for k in range(ep_size)]

        def take(srcs, idx):
            blk = min(1024, srcs[0].shape[0])
            return gather_rows(srcs, idx, blk, 2 * cap, 16).reshape(local_exp, cap, width)

        def fold(keep, send):
            return (keep.astype(jnp.float32) + send.astype(jnp.float32)).astype(jnp.bfloat16)

        sent = []
        for k in range(ep_size):
            mine = tables[k]
            if k:
                last = sent[k - 1][-1]
                mine, held = lax.optimization_barrier((mine, last[0]))
                sent[k - 1][-1] = (held,) + last[1:]
            tok = jnp.maximum(mine[:, 0].astype(jnp.int32) - 1, 0).reshape(-1)
            tok_x = tok if k < 2 else ((tok // part_rows) ^ tp_id) * part_rows + tok % part_rows
            gate_k = mine[:, 1].reshape(local_exp, cap, 1)
            xr = take(x_rows[k], tok_x)
            dr = take(dy_rows[k], tok)
            units = 2 if k == 0 else 1
            count = local_exp // units
            got = []
            for unit in range(units):
                bufs, parts = ffn_call(k, unit * count, count, ep_size, tp_vec, xr, dr, gate_k, scale_row, gate_loc, lin_loc, out_loc, bufs, 512)
                got.append((parts[0], swap_tp(parts[1]), parts[2], swap_tp(parts[3])))
            sent.append(got)
        u_slot, do_slot, h_slot, da_slot, db_slot = bufs
        d_gate = jnp.einsum('sxcd,sxcf->xdf', u_slot, da_slot, preferred_element_type=jnp.float32)
        d_lin = jnp.einsum('sxcd,sxcf->xdf', u_slot, db_slot, preferred_element_type=jnp.float32)
        d_out = jnp.einsum('sxcf,sxcd->xfd', h_slot, do_slot, preferred_element_type=jnp.float32)

        def after(held, *arrs):
            out = lax.optimization_barrier((*arrs, held))
            return out[:-1]

        tail = sent[-1][0][0]
        for k in range(ep_size - 1):
            for unit, (keep_o, got_o, keep_d, got_d) in enumerate(sent[k]):
                if k == ep_size - 2:
                    got_o, *sums_far = after(tail, got_o, *sums_far)
                    got_d, d_gate = lax.optimization_barrier((got_d, d_gate))
                else:
                    got_o, got_d = after(tail, got_o, got_d)
                sent[k][unit] = (keep_o, got_o, keep_d, got_d)
        keep_o, got_o, keep_d, got_d = sent[-1][0]
        got_o, d_lin = lax.optimization_barrier((got_o, d_lin))
        got_d, d_out = lax.optimization_barrier((got_d, d_out))
        sent[-1] = [(keep_o, got_o, keep_d, got_d)]
        o_back, du_back = [], []
        for k in range(ep_size):
            for keep_o, got_o, keep_d, got_d in sent[k]:
                o_sum = fold(keep_o, got_o)
                o_back.append(swap(o_sum, k) if k else o_sum)
                du_sum = fold(keep_d, got_d)
                du_back.append(swap(du_sum, k) if k else du_sum)

        row_first, row_second = rows[:, 0], rows[:, 1]

        def pick(src, rows):
            return src.at[rows].get(mode='promise_in_bounds')

        half_rows = jax.ShapeDtypeStruct((tok_count, half), jnp.bfloat16)
        o_all = jnp.concatenate(o_back, axis=0).reshape(experts * cap, half)
        y_half, dn_part = rows_call(
            combine_kernel, tp_vec,
            [('half', x_loc), ('half', dy_loc), ('row', pick(o_all, row_first)), ('row', pick(o_all, row_second)), ('row', cols)],
            [half_rows, jax.ShapeDtypeStruct((tok_count, 2), jnp.float32)], tok_count, 1024)
        dn_part = dn_part.T
        dn_other = swap_tp(dn_part)
        dn = (dn_part + dn_other).T

        def join(own, other):
            whole = jax.ShapeDtypeStruct((tok_count, width), jnp.bfloat16)
            return rows_call(join_kernel, tp_vec, [('row', own), ('row', other)], [whole], tok_count, 1024)[0]

        y_other = swap_tp(y_half)
        y_loc = join(y_half, y_other)
        stats = ((sums_own + sums_far[0]) + sums_far[1]) + sums_far[2]
        frac_first = stats[0, :experts] / tokens
        z_loss = Z_COEF * stats[2, 0] / tokens
        aux_loss = AUX_COEF * experts * jnp.sum(frac_first * stats[1, :experts]) / tokens
        aux_row = (AUX_COEF * experts * frac_first).reshape(1, experts)
        du_all = jnp.concatenate(du_back, axis=0).reshape(experts * cap, half)
        du_first = pick(du_all, row_first)
        du_second = pick(du_all, row_second)
        dxn, mix, d_scale_half, d_router_half = rows_call(
          norm_kernel, tp_vec,
          [('half', x_loc), ('row', du_first), ('row', du_second), ('row', prob), ('row', idx_loc), ('row', dn), ('same', aux_row), ('deep', w_router), ('lanes', scale_row), ('row', cols)],
          [jax.ShapeDtypeStruct((tok_count, half), jnp.float32), jax.ShapeDtypeStruct((tok_count, 1), jnp.float32), jax.ShapeDtypeStruct((1, half), jnp.float32), jax.ShapeDtypeStruct((half, experts), jnp.float32)], tok_count, 1024)
        mix = mix.reshape(tok_count)
        mix = ((mix + swap_tp(mix)) / width).reshape(tok_count, 1)
        dx_half = rows_call(dx_kernel, tp_vec, [('half', x_loc), ('half', dy_loc), ('row', dxn), ('row', cols), ('row', mix)], [half_rows], tok_count, 1024)[0]
        dx_loc = join(dx_half, swap_tp(dx_half))
        d_scale_half = d_scale_half.reshape(half)
        both = jnp.concatenate([d_router_half.reshape(-1), d_scale_half])
        both = lax.dynamic_update_slice_in_dim(jnp.zeros((2, both.shape[0]), jnp.float32), both[None], tp_id, 0)
        both = lax.psum(both, ('tp', 'ep'))
        d_router = both[:, :half * experts].reshape(width, experts)
        d_scale = both[:, half * experts:].reshape(width)
        losses = jnp.stack([z_loss, aux_loss])
        return (y_loc, losses, dx_loc, d_scale, d_router, d_gate, d_lin, d_out)

    tok_spec = P('ep', None)
    in_spec = P('ep', None, 'tp')
    out_spec = P('ep', 'tp', None)
    return jax.shard_map(device_body, mesh=mesh, in_specs=(tok_spec, tok_spec, tok_spec, P(), P(), in_spec, in_spec, out_spec), out_specs=(tok_spec, P(), tok_spec, P(), P(), in_spec, in_spec, out_spec), check_vma=False)
```

```python
import functools

import jax
import jax.numpy as jnp
from jax import lax
from jax.experimental import pallas as pl
from jax.experimental.pallas import tpu as pltpu
from jax.sharding import PartitionSpec as P


NORM_EPS = 1e-6
Z_COEF = 0.001
AUX_COEF = 0.01
GELU_A = 0.7978845608028654
GELU_B = 0.044715


def ffn_kernel(tp_ref, x_ref, dy_ref, gate_ref, scale_ref, wg_ref, wl_ref, wo_ref, *refs):
    (u_out, do_out, h_out, da_out, db_out, ok_out, os_out, dk_out, ds_out, u_s, do_s, o_acc, du_acc) = refs[-13:]
    f_id = pl.program_id(1)
    half = ok_out.shape[-1]

    @pl.when(f_id == 0)
    def _():
        gate = gate_ref[0]
        live = jnp.logical_not(gate < 0.0)
        x_wide = x_ref[0].astype(jnp.float32)
        inv = lax.rsqrt(jnp.mean(x_wide * x_wide, axis=-1, keepdims=True) + NORM_EPS)
        u_val = jnp.where(live, (x_wide * inv) * scale_ref[...], 0.0).astype(jnp.bfloat16)
        do_val = jnp.where(live, dy_ref[0].astype(jnp.float32) * gate, 0.0).astype(jnp.bfloat16)
        u_s[...] = u_val
        do_s[...] = do_val
        u_out[0, 0] = u_val
        do_out[0, 0] = do_val

    u_val = u_s[...]
    do_val = do_s[...]
    wg = wg_ref[0]
    wl = wl_ref[0]
    wo = wo_ref[0]
    nn = (((1,), (0,)), ((), ()))
    nt = (((1,), (1,)), ((), ()))
    dot = functools.partial(lax.dot_general, preferred_element_type=jnp.float32)
    a0 = dot(u_val, wg, nn)
    a1 = dot(u_val, wl, nn)
    dh = dot(do_val, wo, nt)
    sq = a0 * a0
    th = jnp.tanh(GELU_A * (a0 + GELU_B * (a0 * sq)))
    cdf = 0.5 + 0.5 * th
    ge = a0 * cdf
    slope = cdf + 0.5 * a0 * ((1.0 - th * th) * (GELU_A + (3.0 * GELU_A * GELU_B) * sq))
    h_val = (ge * a1).astype(jnp.bfloat16)
    da = (dh * a1 * slope).astype(jnp.bfloat16)
    db = (dh * ge).astype(jnp.bfloat16)
    h_out[0, 0] = h_val
    da_out[0, 0] = da
    db_out[0, 0] = db
    o_new = dot(h_val, wo, nn)
    du_new = dot(da, wg, nt) + dot(db, wl, nt)

    o_acc[...] = jnp.where(f_id == 0, 0.0, o_acc[...]) + o_new
    du_acc[...] = jnp.where(f_id == 0, 0.0, du_acc[...]) + du_new

    @pl.when(f_id == pl.num_programs(1) - 1)
    def _():
        first = tp_ref[0] == 0
        for acc, keep, send in ((o_acc, ok_out, os_out), (du_acc, dk_out, ds_out)):
            low = acc[:, :half].astype(jnp.bfloat16)
            high = acc[:, half:].astype(jnp.bfloat16)
            keep[0] = jnp.where(first, low, high)
            send[0] = jnp.where(first, high, low)


def router_kernel(blocks, cap, experts, local_exp, ep_ref, x_ref, idx_ref, scale_ref, wr_ref, prob_ref, col_ref, row_ref, tab_ref, sum_ref, carry, prob_acc, sq_acc):
    step = pl.program_id(0)
    rows = x_ref.shape[0]
    first = idx_ref[:, 0:1]
    second = idx_ref[:, 1:2]
    pair_lane = lax.broadcasted_iota(jnp.int32, (rows, 2 * experts), 1)

    @pl.when(step == 0)
    def _():
        carry[...] = jnp.zeros_like(carry)
        prob_acc[...] = jnp.zeros_like(prob_acc)
        sq_acc[...] = jnp.zeros_like(sq_acc)
        tab_ref[...] = jnp.zeros_like(tab_ref)

    @pl.when(step < blocks)
    def _():
        carry[...] += jnp.sum(jnp.where(first + experts == pair_lane, 1.0, 0.0), axis=0, keepdims=True)

    @pl.when(step >= blocks)
    def _():
        x_wide = x_ref[...].astype(jnp.float32)
        inv = lax.rsqrt(jnp.mean(x_wide * x_wide, axis=-1, keepdims=True) + NORM_EPS)
        u_val = ((x_wide * inv) * scale_ref[...]).astype(jnp.bfloat16)
        logits = jnp.dot(u_val.astype(jnp.float32), wr_ref[...], preferred_element_type=jnp.float32)
        top = jnp.max(logits, axis=-1, keepdims=True)
        log_norm = top + jnp.log(jnp.sum(jnp.exp(logits - top), axis=-1, keepdims=True))
        prob = jnp.exp(logits - log_norm)
        prob_ref[...] = prob
        prob_acc[...] += jnp.sum(prob, axis=0, keepdims=True)
        sq_acc[...] += jnp.sum(log_norm * log_norm, axis=0, keepdims=True)
        lane = lax.broadcasted_iota(jnp.int32, (rows, experts), 1)
        p_first = jnp.sum(jnp.where(first == lane, prob, 0.0), axis=-1, keepdims=True)
        p_second = jnp.sum(jnp.where(second == lane, prob, 0.0), axis=-1, keepdims=True)
        total = p_first + p_second
        n_first = p_first / total
        n_second = p_second / total
        sel_first = first == pair_lane
        sel_second = second + experts == pair_lane
        hits = jnp.where(sel_first | sel_second, 1.0, 0.0)
        below = lax.broadcasted_iota(jnp.int32, (rows, rows), 1) < lax.broadcasted_iota(jnp.int32, (rows, rows), 0)
        ranks = jnp.dot(jnp.where(below, 1.0, 0.0).astype(jnp.bfloat16), hits.astype(jnp.bfloat16), preferred_element_type=jnp.float32) + carry[...]
        carry[...] += jnp.sum(hits, axis=0, keepdims=True)
        pos_first = jnp.sum(jnp.where(sel_first, ranks, 0.0), axis=-1, keepdims=True).astype(jnp.int32)
        pos_second = jnp.sum(jnp.where(sel_second, ranks, 0.0), axis=-1, keepdims=True).astype(jnp.int32)
        for c, (route, pos) in enumerate(((first, pos_first), (second, pos_second))):
            kept = pos < cap
            owner = route // local_exp
            spot = (owner ^ ep_ref[0]) * (local_exp * cap) + (route - owner * local_exp) * cap + pos
            row_ref[:, c:c + 1] = jnp.where(kept, spot, 0)
            col_ref[:, 6 + c:7 + c] = jnp.where(kept, spot % 2, 0).astype(jnp.float32)
            col_ref[:, 2 + c:3 + c] = jnp.where(kept, 1.0, 0.0)
        col_ref[:, 0:1] = n_first
        col_ref[:, 1:2] = n_second
        col_ref[:, 4:5] = inv
        col_ref[:, 5:6] = log_norm
        token = lax.broadcasted_iota(jnp.int32, (rows, 1), 0) + ((step - blocks) * rows + 1)
        tok_hi = (token // 128).astype(jnp.float32)
        tok_lo = (token % 128).astype(jnp.float32)
        wide = lax.broadcasted_iota(jnp.int32, (rows, 5 * experts), 1)
        expert = wide % experts
        place = lax.broadcasted_iota(jnp.int32, (rows, cap), 1)
        for route, pos, gate in ((first, pos_first, n_first), (second, pos_second, n_second)):
            hi = gate.astype(jnp.bfloat16).astype(jnp.float32)
            rest = gate - hi
            mid = rest.astype(jnp.bfloat16).astype(jnp.float32)
            vals = jnp.where(wide < experts, tok_hi, jnp.where(wide < 2 * experts, tok_lo, jnp.where(wide < 3 * experts, hi, jnp.where(wide < 4 * experts, mid, rest - mid))))
            left = jnp.where(expert == route, vals, 0.0).astype(jnp.bfloat16)
            right = jnp.where(place == pos, 1.0, 0.0).astype(jnp.bfloat16)
            tab_ref[...] += lax.dot_general(left, right, (((0,), (0,)), ((), ())), preferred_element_type=jnp.float32)

    @pl.when(step == 2 * blocks - 1)
    def _():
        sum_ref[...] = jnp.zeros_like(sum_ref)
        sum_ref[0:1, 0:experts] = carry[:, :experts]
        sum_ref[1:2, 0:experts] = prob_acc[...]
        sum_ref[2:3, 0:1] = sq_acc[...]


def router_call(ep_vec, x_loc, idx_loc, scale_row, w_router, cap, local_exp, block):
    rows, width = x_loc.shape
    experts = w_router.shape[1]
    blocks = rows // block

    def late(i, ep):
        return jnp.maximum(i - blocks, 0), 0

    def fixed(i, ep):
        return 0, 0

    return pl.pallas_call(
        functools.partial(router_kernel, blocks, cap, experts, local_exp),
        grid_spec=pltpu.PrefetchScalarGridSpec(
            num_scalar_prefetch=1,
            grid=(2 * blocks,),
            in_specs=[
                pl.BlockSpec((block, width), late),
                pl.BlockSpec((block, 2), lambda i, ep: (jnp.where(i < blocks, i, i - blocks), 0)),
                pl.BlockSpec((1, width), fixed),
                pl.BlockSpec((width, experts), fixed),
            ],
            out_specs=[pl.BlockSpec((block, experts), late), pl.BlockSpec((block, 8), late), pl.BlockSpec((block, 2), late), pl.BlockSpec((5 * experts, cap), fixed), pl.BlockSpec((8, 128), fixed)],
            scratch_shapes=[pltpu.VMEM((1, 2 * experts), jnp.float32), pltpu.VMEM((1, experts), jnp.float32), pltpu.VMEM((1, 1), jnp.float32)],
        ),
        out_shape=[
            jax.ShapeDtypeStruct((rows, experts), jnp.float32),
            jax.ShapeDtypeStruct((rows, 8), jnp.float32),
            jax.ShapeDtypeStruct((rows, 2), jnp.int32),
            jax.ShapeDtypeStruct((5 * experts, cap), jnp.float32),
            jax.ShapeDtypeStruct((8, 128), jnp.float32),
        ],
        compiler_params=pltpu.CompilerParams(dimension_semantics=("arbitrary",)),
        cost_estimate=pl.CostEstimate(flops=10_000_000_000, bytes_accessed=4 * rows * width, transcendentals=0),
        name="router",
    )(ep_vec, x_loc, idx_loc, scale_row, w_router)


def gather_kernel(parts, fills, blk, rows, group, cols, idx_ref, *refs):
    srcs, out_ref, store, stage = refs[:parts], refs[parts], refs[parts + 1], refs[parts + 2]
    step = pl.program_id(0)
    for p in range(parts):

        @pl.when((step >= p * fills) & (step < (p + 1) * fills))
        def _(p=p):
            val = srcs[p][...].astype(jnp.float32)
            base = pl.multiple_of(step * (blk * 8), blk * 8)
            for j in range(cols):
                store[pl.ds(base + j, blk, stride=8), :] = val[:, j * 128:(j + 1) * 128]

    @pl.when(step >= parts * fills)
    def _():
        start = (step - parts * fills) * rows

        def body(q, carry):
            base = q * group
            vals = [store[pl.ds(pl.multiple_of(idx_ref[start + base + r], 8), 8), :] for r in range(group)]
            for r in range(group):
                stage[pl.ds(pl.multiple_of((base + r) * 8, 8), 8), :] = vals[r]
            return carry

        lax.fori_loop(0, rows // group, body, 0)
        for j in range(cols):
            out_ref[:, j * 128:(j + 1) * 128] = stage[pl.ds(j, rows, stride=8), :].astype(out_ref.dtype)


def gather_rows(srcs, idx, blk, rows, group):
    parts = len(srcs)
    count, width = srcs[0].shape
    fills = count // blk
    total = parts * fills

    def src_map(p, i):
        return jnp.clip(i - p * fills, 0, fills - 1), 0

    return pl.pallas_call(
        functools.partial(gather_kernel, parts, fills, blk, rows, group, width // 128),
        grid=(total + idx.shape[0] // rows,),
        in_specs=[pl.BlockSpec(memory_space=pltpu.SMEM)] + [pl.BlockSpec((blk, width), functools.partial(src_map, p)) for p in range(parts)],
        out_specs=pl.BlockSpec((rows, width), lambda i: (jnp.maximum(i - total, 0), 0)),
        out_shape=jax.ShapeDtypeStruct((idx.shape[0], width), jnp.bfloat16),
        scratch_shapes=[pltpu.VMEM((parts * count * 8, 128), jnp.float32), pltpu.VMEM((rows * 8, 128), jnp.float32)],
        compiler_params=pltpu.CompilerParams(dimension_semantics=("arbitrary",), vmem_limit_bytes=60 * 1024 * 1024),
        cost_estimate=pl.CostEstimate(flops=40_000_000_000, bytes_accessed=4 * width * idx.shape[0], transcendentals=0),
        name="gather_rows",
    )(idx * 8, *srcs)


def combine_kernel(start, pick_first, pick_second, x_ref, dy_ref, col_ref, y_ref, dn_ref):
    col = col_ref[...]
    o1 = jnp.where(col[:, 2:3] > 0.0, pick_first(col[:, 6:7]), 0.0)
    o2 = jnp.where(col[:, 3:4] > 0.0, pick_second(col[:, 7:8]), 0.0)
    y_ref[...] = (x_ref[...].astype(jnp.float32) + col[:, 0:1] * o1 + col[:, 1:2] * o2).astype(y_ref.dtype)
    dy = dy_ref[...].astype(jnp.float32)
    dn_ref[:, 0:1] = jnp.sum(dy * o1, axis=-1, keepdims=True)
    dn_ref[:, 1:2] = jnp.sum(dy * o2, axis=-1, keepdims=True)


def norm_kernel(start, pick_first, pick_second, x_ref, prob_ref, idx_ref, dn_ref, aux_ref, wr_ref, scale_ref, col_ref, dxn_ref, mix_ref, ds_ref, dr_ref):
    col = col_ref[...]
    n_first, n_second = col[:, 0:1], col[:, 1:2]
    dn_first, dn_second = dn_ref[:, 0:1], dn_ref[:, 1:2]
    prob = prob_ref[...]
    aux = aux_ref[...]
    lane = lax.broadcasted_iota(jnp.int32, prob.shape, 1)
    gate_mix = n_first * dn_first + n_second * dn_second
    dl = prob * (aux - jnp.sum(aux * prob, axis=-1, keepdims=True))
    dl = dl + (2.0 * Z_COEF) * col[:, 5:6] * prob
    dl = dl + jnp.where(idx_ref[:, 0:1] == lane, n_first * (dn_first - gate_mix), 0.0)
    dl = dl + jnp.where(idx_ref[:, 1:2] == lane, n_second * (dn_second - gate_mix), 0.0)
    du = jnp.where(col[:, 2:3] > 0.0, pick_first(col[:, 6:7]), 0.0) + jnp.where(col[:, 3:4] > 0.0, pick_second(col[:, 7:8]), 0.0)
    du = du + lax.dot_general(dl, wr_ref[...], (((1,), (1,)), ((), ())), preferred_element_type=jnp.float32)
    xn = x_ref[...].astype(jnp.float32) * col[:, 4:5]
    dxn = du * scale_ref[...]
    dxn_ref[...] = dxn
    mix_ref[...] = jnp.sum(dxn * xn, axis=-1, keepdims=True)
    u_wide = (xn * scale_ref[...]).astype(jnp.bfloat16).astype(jnp.float32)
    ds = jnp.sum(du * xn, axis=0, keepdims=True)
    dr = lax.dot_general(u_wide, dl, (((0,), (0,)), ((), ())), preferred_element_type=jnp.float32)

    @pl.when(pl.program_id(0) == start)
    def _():
        ds_ref[...] = ds
        dr_ref[...] = dr

    @pl.when(pl.program_id(0) > start)
    def _():
        ds_ref[...] += ds
        dr_ref[...] += dr


def dx_kernel(tp_ref, x_ref, dy_ref, dxn_ref, col_ref, mix_ref, dx_ref):
    inv = col_ref[:, 4:5]
    xn = x_ref[...].astype(jnp.float32) * inv
    dx_ref[...] = (dy_ref[...].astype(jnp.float32) + inv * (dxn_ref[...] - xn * mix_ref[...])).astype(dx_ref.dtype)


def join_kernel(tp_ref, own_ref, other_ref, out_ref):
    half = own_ref.shape[1]
    own, other = own_ref[...], other_ref[...]
    first = tp_ref[0] == 0
    out_ref[:, :half] = jnp.where(first, own, other)
    out_ref[:, half:] = jnp.where(first, other, own)


def picking(kernel, parts, fills, blk, group):
    def body(tp_ref, first_ref, second_ref, *refs):
        srcs, rest = refs[:parts], refs[parts:-3]
        store, stage_first, stage_second = refs[-3:]
        step = pl.program_id(0)
        start = parts * fills
        chunks = srcs[0].shape[1] // 128
        rows = stage_first.shape[0] // 8
        for p in range(parts):

            @pl.when((step >= p * fills) & (step < (p + 1) * fills))
            def _(p=p):
                val = srcs[p][...].astype(jnp.float32)
                base = pl.multiple_of(step * (blk * 4), blk * 4)
                for j in range(chunks):
                    store[pl.ds(base + j, blk, stride=4), :] = val[:, j * 128:(j + 1) * 128]

        @pl.when(step >= start)
        def _():
            offset = (step - start) * rows

            def move(q, carry):
                base = q * group
                for idx_ref, stage in ((first_ref, stage_first), (second_ref, stage_second)):
                    vals = [store[pl.ds(pl.multiple_of(idx_ref[offset + base + r], 8), 8), :] for r in range(group)]
                    for r in range(group):
                        stage[pl.ds(pl.multiple_of((base + r) * 8, 8), 8), :] = vals[r]
                return carry

            lax.fori_loop(0, rows // group, move, 0)

            def picker(stage):
                def pick(odd):
                    return jnp.concatenate([jnp.where(odd > 0.0, stage[pl.ds(4 + j, rows, stride=8), :], stage[pl.ds(j, rows, stride=8), :]) for j in range(chunks)], axis=1)

                return pick

            kernel(start, picker(stage_first), picker(stage_second), *rest)

    return body


def rows_call(kernel, tp_vec, ins, outs, rows, block, picks=None):
    specs, args, scalars, scratch, start = [], [], [tp_vec], [], 0
    if picks is not None:
        srcs, first, second = picks
        count, width = srcs[0].shape
        blk = 640
        fills = count // blk
        start = len(srcs) * fills
        kernel = picking(kernel, len(srcs), fills, blk, 16)
        scalars += [first, second]
        for p, src in enumerate(srcs):
            specs.append(pl.BlockSpec((blk, width), functools.partial(lambda p, i, *_: (jnp.clip(i - p * fills, 0, fills - 1), 0), p)))
            args.append(src)
        scratch = [pltpu.VMEM((len(srcs) * count * 4, 128), jnp.float32), pltpu.VMEM((block * 8, 128), jnp.float32), pltpu.VMEM((block * 8, 128), jnp.float32)]

    def at(i):
        return jnp.maximum(i - start, 0) if start else i

    for kind, arr in ins:
        if kind == 'half':
            specs.append(pl.BlockSpec((block, arr.shape[1] // 2), lambda i, tp, *_: (at(i), tp[0])))
        elif kind == 'row':
            specs.append(pl.BlockSpec((block, arr.shape[1]), lambda i, *_: (at(i), 0)))
        elif kind == 'same':
            specs.append(pl.BlockSpec(arr.shape, lambda i, *_: (0, 0)))
        elif kind == 'lanes':
            specs.append(pl.BlockSpec((1, arr.shape[1] // 2), lambda i, tp, *_: (0, tp[0])))
        else:
            specs.append(pl.BlockSpec((arr.shape[0] // 2, arr.shape[1]), lambda i, tp, *_: (tp[0], 0)))
        args.append(arr)
    out_specs = [pl.BlockSpec((block if o.shape[0] == rows else o.shape[0], o.shape[1]), (lambda i, *_: (at(i), 0)) if o.shape[0] == rows else (lambda i, *_: (0, 0))) for o in outs]
    return pl.pallas_call(
        kernel,
        grid_spec=pltpu.PrefetchScalarGridSpec(num_scalar_prefetch=len(scalars), grid=(start + rows // block,), in_specs=specs, out_specs=out_specs, scratch_shapes=scratch),
        out_shape=outs,
        compiler_params=pltpu.CompilerParams(dimension_semantics=("arbitrary",), vmem_limit_bytes=60 * 1024 * 1024),
        cost_estimate=pl.CostEstimate(flops=10_000_000_000, bytes_accessed=sum(a.size * 2 for a in args), transcendentals=0),
    )(*scalars, *args)


def ffn_call(k, base, count, chunks, tp_id, x_rows, dy_rows, gate, scale, wg, wl, wo, bufs, tile):
    experts, rows, width = x_rows.shape
    ff = wg.shape[2]
    steps = ff // tile
    half = width // 2
    row_spec = pl.BlockSpec((1, rows, width), lambda e, f: (base + e, 0, 0))
    in_specs = [
        pl.BlockSpec(memory_space=pltpu.SMEM),
        row_spec,
        row_spec,
        pl.BlockSpec((1, rows, 1), lambda e, f: (base + e, 0, 0)),
        pl.BlockSpec((1, width), lambda e, f: (0, 0)),
        pl.BlockSpec((1, width, tile), lambda e, f: (base + e, 0, f)),
        pl.BlockSpec((1, width, tile), lambda e, f: (base + e, 0, f)),
        pl.BlockSpec((1, tile, width), lambda e, f: (base + e, f, 0)),
    ]
    wide_spec = pl.BlockSpec((1, 1, rows, width), lambda e, f: (k, base + e, 0, 0))
    tile_spec = pl.BlockSpec((1, 1, rows, tile), lambda e, f: (k, base + e, 0, f))
    half_spec = pl.BlockSpec((1, rows, half), lambda e, f: (e, 0, 0))
    wide = jax.ShapeDtypeStruct((chunks, experts, rows, width), jnp.bfloat16)
    deep = jax.ShapeDtypeStruct((chunks, experts, rows, ff), jnp.bfloat16)
    part = jax.ShapeDtypeStruct((count, rows, half), jnp.bfloat16)
    aliases = {}
    if bufs is None:
        bufs = ()
    else:
        aliases = {len(in_specs) + i: i for i in range(5)}
    in_specs = in_specs + [pl.BlockSpec(memory_space=pl.ANY)] * len(bufs)
    flops = 12 * count * rows * width * ff
    outs = pl.pallas_call(
        ffn_kernel,
        grid=(count, steps),
        in_specs=in_specs,
        out_specs=[wide_spec, wide_spec, tile_spec, tile_spec, tile_spec, half_spec, half_spec, half_spec, half_spec],
        out_shape=[wide, wide, deep, deep, deep, part, part, part, part],
        scratch_shapes=[
            pltpu.VMEM((rows, width), jnp.bfloat16),
            pltpu.VMEM((rows, width), jnp.bfloat16),
            pltpu.VMEM((rows, width), jnp.float32),
            pltpu.VMEM((rows, width), jnp.float32),
        ],
        input_output_aliases=aliases,
        compiler_params=pltpu.CompilerParams(dimension_semantics=("arbitrary", "arbitrary"), vmem_limit_bytes=48 * 1024 * 1024),
        cost_estimate=pl.CostEstimate(flops=flops, bytes_accessed=8 * count * rows * (width + ff), transcendentals=count * rows * ff),
        name="ffn",
    )(tp_id, x_rows, dy_rows, gate, scale, wg, wl, wo, *bufs)
    return tuple(outs[:5]), outs[5:]


def solution(mesh):
    ep_size = mesh.shape['ep']

    def swap(arr, k):
        return lax.ppermute(arr, 'ep', [(i, i ^ k) for i in range(ep_size)])

    def swap_tp(arr):
        return lax.ppermute(arr, 'tp', [(0, 1), (1, 0)])

    def device_body(x_loc, dy_loc, idx_loc, norm_scale, w_router, gate_loc, lin_loc, out_loc):
        tok_count, width = x_loc.shape
        experts = w_router.shape[1]
        local_exp = gate_loc.shape[0]
        half = width // 2
        tokens = tok_count * ep_size
        cap = (5 * tok_count + 2 * experts - 1) // (2 * experts)
        ep_id = lax.axis_index('ep')
        tp_id = lax.axis_index('tp')
        tp_vec = tp_id.reshape(1).astype(jnp.int32)
        part_rows = tok_count // 2
        pieces = 2
        piece = part_rows // pieces
        x_near = [swap(lax.dynamic_slice_in_dim(x_loc, tp_id * part_rows + p * piece, piece, 0), 2) for p in range(pieces)]
        dy_far = swap(dy_loc, 2)
        x_side = [swap_tp(x_near[0])]
        x_side.append(swap_tp(x_near[1]))
        x_far = x_near + x_side
        x_rows = [[x_loc], [swap(x_loc, 1)], x_far, [swap(p, 1) for p in x_far]]
        dy_rows = [[dy_loc], [swap(dy_loc, 1)], [dy_far], [swap(dy_far, 1)]]
        scale_row = norm_scale.reshape(1, width)
        prob, cols, rows, tab, sums_own = router_call(ep_id.reshape(1).astype(jnp.int32), x_loc, idx_loc, scale_row, w_router, cap, local_exp, 512)
        tab = tab.reshape(5, experts, cap)
        slot_one = tab[0] * 128.0 + tab[1]
        slot_gate = jnp.where(slot_one > 0.0, (tab[2] + tab[3]) + tab[4], -1.0)
        pair = jnp.stack([slot_one, slot_gate], axis=1).reshape(ep_size, local_exp, 2, cap)
        sums_far = [swap(sums_own, k) for k in range(1, ep_size)]
        bufs = None
        tables = [lax.dynamic_index_in_dim(pair, ep_id ^ k, 0, keepdims=False) for k in range(ep_size)]
        tables = [swap(tables[k], k) if k else tables[k] for k in range(ep_size)]

        def take(srcs, idx):
            blk = min(1024, srcs[0].shape[0])
            return gather_rows(srcs, idx, blk, 2 * cap, 16).reshape(local_exp, cap, width)

        def fold(keep, send):
            return (keep.astype(jnp.float32) + send.astype(jnp.float32)).astype(jnp.bfloat16)

        sent = []
        for k in range(ep_size):
            mine = tables[k]
            if k:
                last = sent[k - 1][-1]
                mine, held = lax.optimization_barrier((mine, last[0]))
                sent[k - 1][-1] = (held,) + last[1:]
            tok = jnp.maximum(mine[:, 0].astype(jnp.int32) - 1, 0).reshape(-1)
            tok_x = tok if k < 2 else ((tok // part_rows) ^ tp_id) * part_rows + tok % part_rows
            gate_k = mine[:, 1].reshape(local_exp, cap, 1)
            xr = take(x_rows[k], tok_x)
            dr = take(dy_rows[k], tok)
            units = 2
            count = local_exp // units
            got = []
            for unit in range(units):
                bufs, parts = ffn_call(k, unit * count, count, ep_size, tp_vec, xr, dr, gate_k, scale_row, gate_loc, lin_loc, out_loc, bufs, 512)
                got.append((parts[0], swap_tp(parts[1]), parts[2], swap_tp(parts[3])))
            sent.append(got)
        u_slot, do_slot, h_slot, da_slot, db_slot = bufs
        d_gate = jnp.einsum('sxcd,sxcf->xdf', u_slot, da_slot, preferred_element_type=jnp.float32)
        d_lin = jnp.einsum('sxcd,sxcf->xdf', u_slot, db_slot, preferred_element_type=jnp.float32)
        d_out = jnp.einsum('sxcf,sxcd->xfd', h_slot, do_slot, preferred_element_type=jnp.float32)

        def after(held, *arrs):
            out = lax.optimization_barrier((*arrs, held))
            return out[:-1]

        tail = sent[-1][-1][0]
        for k in range(ep_size - 2):
            for unit, (keep_o, got_o, keep_d, got_d) in enumerate(sent[k]):
                got_o, = after(tail, got_o)
                got_d, d_out = lax.optimization_barrier((got_d, d_out))
                sent[k][unit] = (keep_o, got_o, keep_d, got_d)
        near = sent[-1][0][0]
        for unit, (keep_o, got_o, keep_d, got_d) in enumerate(sent[-2]):
            got_o, = after(near, got_o)
            if unit:
                got_d, d_gate = lax.optimization_barrier((got_d, d_gate))
            else:
                got_d, = after(near, got_d)
            sent[-2][unit] = (keep_o, got_o, keep_d, got_d)
        sums_far = after(tail, *sums_far)
        for unit in range(2):
            keep_o, got_o, keep_d, got_d = sent[-1][unit]
            got_o, d_gate = lax.optimization_barrier((got_o, d_gate))
            got_d, d_lin = lax.optimization_barrier((got_d, d_lin))
            sent[-1][unit] = (keep_o, got_o, keep_d, got_d)
        o_back, du_back = [], []
        for k in range(ep_size):
            for keep_o, got_o, keep_d, got_d in sent[k]:
                o_sum = fold(keep_o, got_o)
                o_back.append(swap(o_sum, k) if k else o_sum)
                du_sum = fold(keep_d, got_d)
                du_back.append(swap(du_sum, k) if k else du_sum)

        tile_rows = (rows >> 1) * 8
        row_first, row_second = tile_rows[:, 0], tile_rows[:, 1]

        half_rows = jax.ShapeDtypeStruct((tok_count, half), jnp.bfloat16)
        o_parts = [arr.reshape(-1, half) for arr in o_back]
        y_half, dn_part = rows_call(
            combine_kernel, tp_vec, [('half', x_loc), ('half', dy_loc), ('row', cols)],
            [half_rows, jax.ShapeDtypeStruct((tok_count, 2), jnp.float32)], tok_count, 512, (o_parts, row_first, row_second))
        dn_part = dn_part.T
        dn_other = swap_tp(dn_part)
        dn = (dn_part + dn_other).T

        def join(own, other):
            whole = jax.ShapeDtypeStruct((tok_count, width), jnp.bfloat16)
            return rows_call(join_kernel, tp_vec, [('row', own), ('row', other)], [whole], tok_count, 1024)[0]

        y_other = swap_tp(y_half)
        y_loc = join(y_half, y_other)
        stats = ((sums_own + sums_far[0]) + sums_far[1]) + sums_far[2]
        frac_first = stats[0, :experts] / tokens
        z_loss = Z_COEF * stats[2, 0] / tokens
        aux_loss = AUX_COEF * experts * jnp.sum(frac_first * stats[1, :experts]) / tokens
        aux_row = (AUX_COEF * experts * frac_first).reshape(1, experts)
        du_parts = [arr.reshape(-1, half) for arr in du_back]
        dxn, mix, d_scale_half, d_router_half = rows_call(
            norm_kernel, tp_vec,
            [('half', x_loc), ('row', prob), ('row', idx_loc), ('row', dn), ('same', aux_row), ('deep', w_router), ('lanes', scale_row), ('row', cols)],
            [jax.ShapeDtypeStruct((tok_count, half), jnp.float32), jax.ShapeDtypeStruct((tok_count, 1), jnp.float32), jax.ShapeDtypeStruct((1, half), jnp.float32), jax.ShapeDtypeStruct((half, experts), jnp.float32)],
            tok_count, 512, (du_parts, row_first, row_second))
        mix = mix.reshape(tok_count)
        mix = ((mix + swap_tp(mix)) / width).reshape(tok_count, 1)
        dx_half = rows_call(dx_kernel, tp_vec, [('half', x_loc), ('half', dy_loc), ('row', dxn), ('row', cols), ('row', mix)], [half_rows], tok_count, 1024)[0]
        dx_loc = join(dx_half, swap_tp(dx_half))
        d_scale_half = d_scale_half.reshape(half)
        both = jnp.concatenate([d_router_half.reshape(-1), d_scale_half])
        both = lax.dynamic_update_slice_in_dim(jnp.zeros((2, both.shape[0]), jnp.float32), both[None], tp_id, 0)
        both = lax.psum(both, ('tp', 'ep'))
        d_router = both[:, :half * experts].reshape(width, experts)
        d_scale = both[:, half * experts:].reshape(width)
        losses = jnp.stack([z_loss, aux_loss])
        return (y_loc, losses, dx_loc, d_scale, d_router, d_gate, d_lin, d_out)

    tok_spec = P('ep', None)
    in_spec = P('ep', None, 'tp')
    out_spec = P('ep', 'tp', None)
    return jax.shard_map(device_body, mesh=mesh, in_specs=(tok_spec, tok_spec, tok_spec, P(), P(), in_spec, in_spec, out_spec), out_specs=(tok_spec, P(), tok_spec, P(), P(), in_spec, in_spec, out_spec), check_vma=False)
```

```python
import functools

import jax
import jax.numpy as jnp
from jax import lax
from jax.experimental import pallas as pl
from jax.experimental.pallas import tpu as pltpu
from jax.sharding import PartitionSpec as P


NORM_EPS = 1e-6
Z_COEF = 0.001
AUX_COEF = 0.01
GELU_A = 0.7978845608028654
GELU_B = 0.044715


def ffn_kernel(tp_ref, x_ref, dy_ref, gate_ref, scale_ref, wg_ref, wl_ref, wo_ref, *refs):
    (u_out, do_out, h_out, da_out, db_out, ok_out, os_out, dk_out, ds_out, u_s, do_s, o_acc, du_acc) = refs[-13:]
    f_id = pl.program_id(1)
    half = ok_out.shape[-1]

    @pl.when(f_id == 0)
    def _():
        gate = gate_ref[0]
        live = jnp.logical_not(gate < 0.0)
        x_wide = x_ref[0].astype(jnp.float32)
        inv = lax.rsqrt(jnp.mean(x_wide * x_wide, axis=-1, keepdims=True) + NORM_EPS)
        u_val = jnp.where(live, (x_wide * inv) * scale_ref[...], 0.0).astype(jnp.bfloat16)
        do_val = jnp.where(live, dy_ref[0].astype(jnp.float32) * gate, 0.0).astype(jnp.bfloat16)
        u_s[...] = u_val
        do_s[...] = do_val
        u_out[0, 0] = u_val
        do_out[0, 0] = do_val

    u_val = u_s[...]
    do_val = do_s[...]
    wg = wg_ref[0]
    wl = wl_ref[0]
    wo = wo_ref[0]
    nn = (((1,), (0,)), ((), ()))
    nt = (((1,), (1,)), ((), ()))
    dot = functools.partial(lax.dot_general, preferred_element_type=jnp.float32)
    a0 = dot(u_val, wg, nn)
    a1 = dot(u_val, wl, nn)
    dh = dot(do_val, wo, nt)
    sq = a0 * a0
    th = jnp.tanh(GELU_A * (a0 + GELU_B * (a0 * sq)))
    cdf = 0.5 + 0.5 * th
    ge = a0 * cdf
    slope = cdf + 0.5 * a0 * ((1.0 - th * th) * (GELU_A + (3.0 * GELU_A * GELU_B) * sq))
    h_val = (ge * a1).astype(jnp.bfloat16)
    da = (dh * a1 * slope).astype(jnp.bfloat16)
    db = (dh * ge).astype(jnp.bfloat16)
    h_out[0, 0] = h_val
    da_out[0, 0] = da
    db_out[0, 0] = db
    o_new = dot(h_val, wo, nn)
    du_new = dot(da, wg, nt) + dot(db, wl, nt)

    o_acc[...] = jnp.where(f_id == 0, 0.0, o_acc[...]) + o_new
    du_acc[...] = jnp.where(f_id == 0, 0.0, du_acc[...]) + du_new

    @pl.when(f_id == pl.num_programs(1) - 1)
    def _():
        first = tp_ref[0] == 0
        for acc, keep, send in ((o_acc, ok_out, os_out), (du_acc, dk_out, ds_out)):
            low = acc[:, :half].astype(jnp.bfloat16)
            high = acc[:, half:].astype(jnp.bfloat16)
            keep[0] = jnp.where(first, low, high)
            send[0] = jnp.where(first, high, low)


def router_kernel(blocks, cap, experts, local_exp, ep_ref, x_ref, idx_ref, scale_ref, wr_ref, prob_ref, col_ref, row_ref, tab_ref, sum_ref, carry, prob_acc, sq_acc):
    step = pl.program_id(0)
    rows = x_ref.shape[0]
    first = idx_ref[:, 0:1]
    second = idx_ref[:, 1:2]
    pair_lane = lax.broadcasted_iota(jnp.int32, (rows, 2 * experts), 1)

    @pl.when(step == 0)
    def _():
        carry[...] = jnp.zeros_like(carry)
        prob_acc[...] = jnp.zeros_like(prob_acc)
        sq_acc[...] = jnp.zeros_like(sq_acc)
        tab_ref[...] = jnp.zeros_like(tab_ref)

    @pl.when(step < blocks)
    def _():
        carry[...] += jnp.sum(jnp.where(first + experts == pair_lane, 1.0, 0.0), axis=0, keepdims=True)

    @pl.when(step >= blocks)
    def _():
        x_wide = x_ref[...].astype(jnp.float32)
        inv = lax.rsqrt(jnp.mean(x_wide * x_wide, axis=-1, keepdims=True) + NORM_EPS)
        u_val = ((x_wide * inv) * scale_ref[...]).astype(jnp.bfloat16)
        logits = jnp.dot(u_val.astype(jnp.float32), wr_ref[...], preferred_element_type=jnp.float32)
        top = jnp.max(logits, axis=-1, keepdims=True)
        log_norm = top + jnp.log(jnp.sum(jnp.exp(logits - top), axis=-1, keepdims=True))
        prob = jnp.exp(logits - log_norm)
        prob_ref[...] = prob
        prob_acc[...] += jnp.sum(prob, axis=0, keepdims=True)
        sq_acc[...] += jnp.sum(log_norm * log_norm, axis=0, keepdims=True)
        lane = lax.broadcasted_iota(jnp.int32, (rows, experts), 1)
        p_first = jnp.sum(jnp.where(first == lane, prob, 0.0), axis=-1, keepdims=True)
        p_second = jnp.sum(jnp.where(second == lane, prob, 0.0), axis=-1, keepdims=True)
        total = p_first + p_second
        n_first = p_first / total
        n_second = p_second / total
        sel_first = first == pair_lane
        sel_second = second + experts == pair_lane
        hits = jnp.where(sel_first | sel_second, 1.0, 0.0)
        below = lax.broadcasted_iota(jnp.int32, (rows, rows), 1) < lax.broadcasted_iota(jnp.int32, (rows, rows), 0)
        ranks = jnp.dot(jnp.where(below, 1.0, 0.0).astype(jnp.bfloat16), hits.astype(jnp.bfloat16), preferred_element_type=jnp.float32) + carry[...]
        carry[...] += jnp.sum(hits, axis=0, keepdims=True)
        pos_first = jnp.sum(jnp.where(sel_first, ranks, 0.0), axis=-1, keepdims=True).astype(jnp.int32)
        pos_second = jnp.sum(jnp.where(sel_second, ranks, 0.0), axis=-1, keepdims=True).astype(jnp.int32)
        for c, (route, pos) in enumerate(((first, pos_first), (second, pos_second))):
            kept = pos < cap
            owner = route // local_exp
            spot = (owner ^ ep_ref[0]) * (local_exp * cap) + (route - owner * local_exp) * cap + pos
            row_ref[:, c:c + 1] = jnp.where(kept, spot, 0)
            col_ref[:, 6 + c:7 + c] = jnp.where(kept, spot % 2, 0).astype(jnp.float32)
            col_ref[:, 2 + c:3 + c] = jnp.where(kept, 1.0, 0.0)
        col_ref[:, 0:1] = n_first
        col_ref[:, 1:2] = n_second
        col_ref[:, 4:5] = inv
        col_ref[:, 5:6] = log_norm
        token = lax.broadcasted_iota(jnp.int32, (rows, 1), 0) + ((step - blocks) * rows + 1)
        tok_hi = (token // 128).astype(jnp.float32)
        tok_lo = (token % 128).astype(jnp.float32)
        wide = lax.broadcasted_iota(jnp.int32, (rows, 5 * experts), 1)
        expert = wide % experts
        place = lax.broadcasted_iota(jnp.int32, (rows, cap), 1)
        for route, pos, gate in ((first, pos_first, n_first), (second, pos_second, n_second)):
            hi = gate.astype(jnp.bfloat16).astype(jnp.float32)
            rest = gate - hi
            mid = rest.astype(jnp.bfloat16).astype(jnp.float32)
            vals = jnp.where(wide < experts, tok_hi, jnp.where(wide < 2 * experts, tok_lo, jnp.where(wide < 3 * experts, hi, jnp.where(wide < 4 * experts, mid, rest - mid))))
            left = jnp.where(expert == route, vals, 0.0).astype(jnp.bfloat16)
            right = jnp.where(place == pos, 1.0, 0.0).astype(jnp.bfloat16)
            tab_ref[...] += lax.dot_general(left, right, (((0,), (0,)), ((), ())), preferred_element_type=jnp.float32)

    @pl.when(step == 2 * blocks - 1)
    def _():
        sum_ref[...] = jnp.zeros_like(sum_ref)
        sum_ref[0:1, 0:experts] = carry[:, :experts]
        sum_ref[1:2, 0:experts] = prob_acc[...]
        sum_ref[2:3, 0:1] = sq_acc[...]


def router_call(ep_vec, x_loc, idx_loc, scale_row, w_router, cap, local_exp, block):
    rows, width = x_loc.shape
    experts = w_router.shape[1]
    blocks = rows // block

    def late(i, ep):
        return jnp.maximum(i - blocks, 0), 0

    def fixed(i, ep):
        return 0, 0

    return pl.pallas_call(
        functools.partial(router_kernel, blocks, cap, experts, local_exp),
        grid_spec=pltpu.PrefetchScalarGridSpec(
            num_scalar_prefetch=1,
            grid=(2 * blocks,),
            in_specs=[
                pl.BlockSpec((block, width), late),
                pl.BlockSpec((block, 2), lambda i, ep: (jnp.where(i < blocks, i, i - blocks), 0)),
                pl.BlockSpec((1, width), fixed),
                pl.BlockSpec((width, experts), fixed),
            ],
            out_specs=[pl.BlockSpec((block, experts), late), pl.BlockSpec((block, 8), late), pl.BlockSpec((block, 2), late), pl.BlockSpec((5 * experts, cap), fixed), pl.BlockSpec((8, 128), fixed)],
            scratch_shapes=[pltpu.VMEM((1, 2 * experts), jnp.float32), pltpu.VMEM((1, experts), jnp.float32), pltpu.VMEM((1, 1), jnp.float32)],
        ),
        out_shape=[
            jax.ShapeDtypeStruct((rows, experts), jnp.float32),
            jax.ShapeDtypeStruct((rows, 8), jnp.float32),
            jax.ShapeDtypeStruct((rows, 2), jnp.int32),
            jax.ShapeDtypeStruct((5 * experts, cap), jnp.float32),
            jax.ShapeDtypeStruct((8, 128), jnp.float32),
        ],
        compiler_params=pltpu.CompilerParams(dimension_semantics=("arbitrary",)),
        cost_estimate=pl.CostEstimate(flops=10_000_000_000, bytes_accessed=4 * rows * width, transcendentals=0),
        name="router",
    )(ep_vec, x_loc, idx_loc, scale_row, w_router)


def gather_kernel(parts, fills, blk, rows, group, cols, idx_ref, *refs):
    srcs, out_ref, store, stage = refs[:parts], refs[parts], refs[parts + 1], refs[parts + 2]
    step = pl.program_id(0)
    for p in range(parts):

        @pl.when((step >= p * fills) & (step < (p + 1) * fills))
        def _(p=p):
            val = srcs[p][...].astype(jnp.float32)
            base = pl.multiple_of(step * (blk * 8), blk * 8)
            for j in range(cols):
                store[pl.ds(base + j, blk, stride=8), :] = val[:, j * 128:(j + 1) * 128]

    @pl.when(step >= parts * fills)
    def _():
        start = (step - parts * fills) * rows

        def body(q, carry):
            base = q * group
            vals = [store[pl.ds(pl.multiple_of(idx_ref[start + base + r], 8), 8), :] for r in range(group)]
            for r in range(group):
                stage[pl.ds(pl.multiple_of((base + r) * 8, 8), 8), :] = vals[r]
            return carry

        lax.fori_loop(0, rows // group, body, 0)
        for j in range(cols):
            out_ref[:, j * 128:(j + 1) * 128] = stage[pl.ds(j, rows, stride=8), :].astype(out_ref.dtype)


def gather_rows(srcs, idx, blk, rows, group):
    parts = len(srcs)
    count, width = srcs[0].shape
    fills = count // blk
    total = parts * fills

    def src_map(p, i):
        return jnp.clip(i - p * fills, 0, fills - 1), 0

    return pl.pallas_call(
        functools.partial(gather_kernel, parts, fills, blk, rows, group, width // 128),
        grid=(total + idx.shape[0] // rows,),
        in_specs=[pl.BlockSpec(memory_space=pltpu.SMEM)] + [pl.BlockSpec((blk, width), functools.partial(src_map, p)) for p in range(parts)],
        out_specs=pl.BlockSpec((rows, width), lambda i: (jnp.maximum(i - total, 0), 0)),
        out_shape=jax.ShapeDtypeStruct((idx.shape[0], width), jnp.bfloat16),
        scratch_shapes=[pltpu.VMEM((parts * count * 8, 128), jnp.float32), pltpu.VMEM((rows * 8, 128), jnp.float32)],
        compiler_params=pltpu.CompilerParams(dimension_semantics=("arbitrary",), vmem_limit_bytes=60 * 1024 * 1024),
        cost_estimate=pl.CostEstimate(flops=40_000_000_000, bytes_accessed=4 * width * idx.shape[0], transcendentals=0),
        name="gather_rows",
    )(idx * 8, *srcs)


def combine_kernel(start, pick_first, pick_second, x_ref, dy_ref, col_ref, y_ref, dn_ref):
    col = col_ref[...]
    o1 = jnp.where(col[:, 2:3] > 0.0, pick_first(col[:, 6:7]), 0.0)
    o2 = jnp.where(col[:, 3:4] > 0.0, pick_second(col[:, 7:8]), 0.0)
    y_ref[...] = (x_ref[...].astype(jnp.float32) + col[:, 0:1] * o1 + col[:, 1:2] * o2).astype(y_ref.dtype)
    dy = dy_ref[...].astype(jnp.float32)
    dn_ref[:, 0:1] = jnp.sum(dy * o1, axis=-1, keepdims=True)
    dn_ref[:, 1:2] = jnp.sum(dy * o2, axis=-1, keepdims=True)


def norm_kernel(start, pick_first, pick_second, x_ref, prob_ref, idx_ref, dn_ref, aux_ref, wr_ref, scale_ref, col_ref, dxn_ref, mix_ref, ds_ref, dr_ref):
    col = col_ref[...]
    n_first, n_second = col[:, 0:1], col[:, 1:2]
    dn_first, dn_second = dn_ref[:, 0:1], dn_ref[:, 1:2]
    prob = prob_ref[...]
    aux = aux_ref[...]
    lane = lax.broadcasted_iota(jnp.int32, prob.shape, 1)
    gate_mix = n_first * dn_first + n_second * dn_second
    dl = prob * (aux - jnp.sum(aux * prob, axis=-1, keepdims=True))
    dl = dl + (2.0 * Z_COEF) * col[:, 5:6] * prob
    dl = dl + jnp.where(idx_ref[:, 0:1] == lane, n_first * (dn_first - gate_mix), 0.0)
    dl = dl + jnp.where(idx_ref[:, 1:2] == lane, n_second * (dn_second - gate_mix), 0.0)
    du = jnp.where(col[:, 2:3] > 0.0, pick_first(col[:, 6:7]), 0.0) + jnp.where(col[:, 3:4] > 0.0, pick_second(col[:, 7:8]), 0.0)
    du = du + lax.dot_general(dl, wr_ref[...], (((1,), (1,)), ((), ())), preferred_element_type=jnp.float32)
    xn = x_ref[...].astype(jnp.float32) * col[:, 4:5]
    dxn = du * scale_ref[...]
    dxn_ref[...] = dxn
    mix_ref[...] = jnp.sum(dxn * xn, axis=-1, keepdims=True)
    u_wide = (xn * scale_ref[...]).astype(jnp.bfloat16).astype(jnp.float32)
    ds = jnp.sum(du * xn, axis=0, keepdims=True)
    dr = lax.dot_general(u_wide, dl, (((0,), (0,)), ((), ())), preferred_element_type=jnp.float32)

    @pl.when(pl.program_id(0) == start)
    def _():
        ds_ref[...] = ds
        dr_ref[...] = dr

    @pl.when(pl.program_id(0) > start)
    def _():
        ds_ref[...] += ds
        dr_ref[...] += dr


def dx_kernel(tp_ref, x_ref, dy_ref, dxn_ref, col_ref, mix_ref, dx_ref):
    inv = col_ref[:, 4:5]
    xn = x_ref[...].astype(jnp.float32) * inv
    dx_ref[...] = (dy_ref[...].astype(jnp.float32) + inv * (dxn_ref[...] - xn * mix_ref[...])).astype(dx_ref.dtype)


def join_kernel(tp_ref, own_ref, other_ref, out_ref):
    half = own_ref.shape[1]
    own, other = own_ref[...], other_ref[...]
    first = tp_ref[0] == 0
    out_ref[:, :half] = jnp.where(first, own, other)
    out_ref[:, half:] = jnp.where(first, other, own)


def picking(kernel, parts, fills, blk, group):
    def body(tp_ref, first_ref, second_ref, *refs):
        srcs, rest = refs[:parts], refs[parts:-3]
        store, stage_first, stage_second = refs[-3:]
        step = pl.program_id(0)
        start = parts * fills
        chunks = srcs[0].shape[1] // 128
        rows = stage_first.shape[0] // 8
        for p in range(parts):

            @pl.when((step >= p * fills) & (step < (p + 1) * fills))
            def _(p=p):
                val = srcs[p][...].astype(jnp.float32)
                base = pl.multiple_of(step * (blk * 4), blk * 4)
                for j in range(chunks):
                    store[pl.ds(base + j, blk, stride=4), :] = val[:, j * 128:(j + 1) * 128]

        @pl.when(step >= start)
        def _():
            offset = (step - start) * rows

            def move(q, carry):
                base = q * group
                for idx_ref, stage in ((first_ref, stage_first), (second_ref, stage_second)):
                    vals = [store[pl.ds(pl.multiple_of(idx_ref[offset + base + r], 8), 8), :] for r in range(group)]
                    for r in range(group):
                        stage[pl.ds(pl.multiple_of((base + r) * 8, 8), 8), :] = vals[r]
                return carry

            lax.fori_loop(0, rows // group, move, 0)

            def picker(stage):
                def pick(odd):
                    return jnp.concatenate([jnp.where(odd > 0.0, stage[pl.ds(4 + j, rows, stride=8), :], stage[pl.ds(j, rows, stride=8), :]) for j in range(chunks)], axis=1)

                return pick

            kernel(start, picker(stage_first), picker(stage_second), *rest)

    return body


def rows_call(kernel, tp_vec, ins, outs, rows, block, picks=None):
    specs, args, scalars, scratch, start = [], [], [tp_vec], [], 0
    if picks is not None:
        srcs, first, second = picks
        count, width = srcs[0].shape
        blk = 640
        fills = count // blk
        start = len(srcs) * fills
        kernel = picking(kernel, len(srcs), fills, blk, 16)
        scalars += [first, second]
        for p, src in enumerate(srcs):
            specs.append(pl.BlockSpec((blk, width), functools.partial(lambda p, i, *_: (jnp.clip(i - p * fills, 0, fills - 1), 0), p)))
            args.append(src)
        scratch = [pltpu.VMEM((len(srcs) * count * 4, 128), jnp.float32), pltpu.VMEM((block * 8, 128), jnp.float32), pltpu.VMEM((block * 8, 128), jnp.float32)]

    def at(i):
        return jnp.maximum(i - start, 0) if start else i

    for kind, arr in ins:
        if kind == 'half':
            specs.append(pl.BlockSpec((block, arr.shape[1] // 2), lambda i, tp, *_: (at(i), tp[0])))
        elif kind == 'row':
            specs.append(pl.BlockSpec((block, arr.shape[1]), lambda i, *_: (at(i), 0)))
        elif kind == 'same':
            specs.append(pl.BlockSpec(arr.shape, lambda i, *_: (0, 0)))
        elif kind == 'lanes':
            specs.append(pl.BlockSpec((1, arr.shape[1] // 2), lambda i, tp, *_: (0, tp[0])))
        else:
            specs.append(pl.BlockSpec((arr.shape[0] // 2, arr.shape[1]), lambda i, tp, *_: (tp[0], 0)))
        args.append(arr)
    out_specs = [pl.BlockSpec((block if o.shape[0] == rows else o.shape[0], o.shape[1]), (lambda i, *_: (at(i), 0)) if o.shape[0] == rows else (lambda i, *_: (0, 0))) for o in outs]
    return pl.pallas_call(
        kernel,
        grid_spec=pltpu.PrefetchScalarGridSpec(num_scalar_prefetch=len(scalars), grid=(start + rows // block,), in_specs=specs, out_specs=out_specs, scratch_shapes=scratch),
        out_shape=outs,
        compiler_params=pltpu.CompilerParams(dimension_semantics=("arbitrary",), vmem_limit_bytes=60 * 1024 * 1024),
        cost_estimate=pl.CostEstimate(flops=10_000_000_000, bytes_accessed=sum(a.size * 2 for a in args), transcendentals=0),
    )(*scalars, *args)


def ffn_call(k, base, count, chunks, tp_id, x_rows, dy_rows, gate, scale, wg, wl, wo, bufs, tile):
    experts, rows, width = x_rows.shape
    ff = wg.shape[2]
    steps = ff // tile
    half = width // 2
    row_spec = pl.BlockSpec((1, rows, width), lambda e, f: (base + e, 0, 0))
    in_specs = [
        pl.BlockSpec(memory_space=pltpu.SMEM),
        row_spec,
        row_spec,
        pl.BlockSpec((1, rows, 1), lambda e, f: (base + e, 0, 0)),
        pl.BlockSpec((1, width), lambda e, f: (0, 0)),
        pl.BlockSpec((1, width, tile), lambda e, f: (base + e, 0, f)),
        pl.BlockSpec((1, width, tile), lambda e, f: (base + e, 0, f)),
        pl.BlockSpec((1, tile, width), lambda e, f: (base + e, f, 0)),
    ]
    wide_spec = pl.BlockSpec((1, 1, rows, width), lambda e, f: (k, base + e, 0, 0))
    tile_spec = pl.BlockSpec((1, 1, rows, tile), lambda e, f: (k, base + e, 0, f))
    half_spec = pl.BlockSpec((1, rows, half), lambda e, f: (e, 0, 0))
    wide = jax.ShapeDtypeStruct((chunks, experts, rows, width), jnp.bfloat16)
    deep = jax.ShapeDtypeStruct((chunks, experts, rows, ff), jnp.bfloat16)
    part = jax.ShapeDtypeStruct((count, rows, half), jnp.bfloat16)
    aliases = {}
    if bufs is None:
        bufs = ()
    else:
        aliases = {len(in_specs) + i: i for i in range(5)}
    in_specs = in_specs + [pl.BlockSpec(memory_space=pl.ANY)] * len(bufs)
    flops = 12 * count * rows * width * ff
    outs = pl.pallas_call(
        ffn_kernel,
        grid=(count, steps),
        in_specs=in_specs,
        out_specs=[wide_spec, wide_spec, tile_spec, tile_spec, tile_spec, half_spec, half_spec, half_spec, half_spec],
        out_shape=[wide, wide, deep, deep, deep, part, part, part, part],
        scratch_shapes=[
            pltpu.VMEM((rows, width), jnp.bfloat16),
            pltpu.VMEM((rows, width), jnp.bfloat16),
            pltpu.VMEM((rows, width), jnp.float32),
            pltpu.VMEM((rows, width), jnp.float32),
        ],
        input_output_aliases=aliases,
        compiler_params=pltpu.CompilerParams(dimension_semantics=("arbitrary", "arbitrary"), vmem_limit_bytes=48 * 1024 * 1024),
        cost_estimate=pl.CostEstimate(flops=flops, bytes_accessed=8 * count * rows * (width + ff), transcendentals=count * rows * ff),
        name="ffn",
    )(tp_id, x_rows, dy_rows, gate, scale, wg, wl, wo, *bufs)
    return tuple(outs[:5]), outs[5:]


def solution(mesh):
    ep_size = mesh.shape['ep']

    def swap(arr, k):
        return lax.ppermute(arr, 'ep', [(i, i ^ k) for i in range(ep_size)])

    def swap_tp(arr):
        return lax.ppermute(arr, 'tp', [(0, 1), (1, 0)])

    def device_body(x_loc, dy_loc, idx_loc, norm_scale, w_router, gate_loc, lin_loc, out_loc):
        tok_count, width = x_loc.shape
        experts = w_router.shape[1]
        local_exp = gate_loc.shape[0]
        half = width // 2
        tokens = tok_count * ep_size
        cap = (5 * tok_count + 2 * experts - 1) // (2 * experts)
        ep_id = lax.axis_index('ep')
        tp_id = lax.axis_index('tp')
        tp_vec = tp_id.reshape(1).astype(jnp.int32)
        part_rows = tok_count // 2
        pieces = 2
        piece = part_rows // pieces
        x_near = [swap(lax.dynamic_slice_in_dim(x_loc, tp_id * part_rows + p * piece, piece, 0), 2) for p in range(pieces)]
        dy_far = swap(dy_loc, 2)
        x_side = [swap_tp(x_near[0])]
        x_side.append(swap_tp(x_near[1]))
        x_far = x_near + x_side
        x_rows = [[x_loc], [swap(x_loc, 1)], x_far, [swap(p, 1) for p in x_far]]
        dy_rows = [[dy_loc], [swap(dy_loc, 1)], [dy_far], [swap(dy_far, 1)]]
        scale_row = norm_scale.reshape(1, width)
        prob, cols, rows, tab, sums_own = router_call(ep_id.reshape(1).astype(jnp.int32), x_loc, idx_loc, scale_row, w_router, cap, local_exp, 512)
        tab = tab.reshape(5, experts, cap)
        slot_one = tab[0] * 128.0 + tab[1]
        slot_gate = jnp.where(slot_one > 0.0, (tab[2] + tab[3]) + tab[4], -1.0)
        pair = jnp.stack([slot_one, slot_gate], axis=1).reshape(ep_size, local_exp, 2, cap)
        sums_far = [swap(sums_own, k) for k in range(1, ep_size)]
        bufs = None
        tables = [lax.dynamic_index_in_dim(pair, ep_id ^ k, 0, keepdims=False) for k in range(ep_size)]
        tables = [swap(tables[k], k) if k else tables[k] for k in range(ep_size)]

        def take(srcs, idx):
            blk = min(1024, srcs[0].shape[0])
            return gather_rows(srcs, idx, blk, 2 * cap, 16).reshape(local_exp, cap, width)

        def fold(keep, send):
            return (keep.astype(jnp.float32) + send.astype(jnp.float32)).astype(jnp.bfloat16)

        sent = []
        for k in range(ep_size):
            mine = tables[k]
            if k:
                last = sent[k - 1][-1]
                mine, held = lax.optimization_barrier((mine, last[0]))
                sent[k - 1][-1] = (held,) + last[1:]
            tok = jnp.maximum(mine[:, 0].astype(jnp.int32) - 1, 0).reshape(-1)
            tok_x = tok if k < 2 else ((tok // part_rows) ^ tp_id) * part_rows + tok % part_rows
            gate_k = mine[:, 1].reshape(local_exp, cap, 1)
            xr = take(x_rows[k], tok_x)
            dr = take(dy_rows[k], tok)
            units = 2
            count = local_exp // units
            got = []
            for unit in range(units):
                bufs, parts = ffn_call(k, unit * count, count, ep_size, tp_vec, xr, dr, gate_k, scale_row, gate_loc, lin_loc, out_loc, bufs, 512)
                got.append((parts[0], swap_tp(parts[1]), parts[2], swap_tp(parts[3])))
            sent.append(got)
        u_slot, do_slot, h_slot, da_slot, db_slot = bufs
        d_gate = jnp.einsum('sxcd,sxcf->xdf', u_slot, da_slot, preferred_element_type=jnp.float32)
        d_lin = jnp.einsum('sxcd,sxcf->xdf', u_slot, db_slot, preferred_element_type=jnp.float32)
        d_out = jnp.einsum('sxcf,sxcd->xfd', h_slot, do_slot, preferred_element_type=jnp.float32)

        def after(held, *arrs):
            out = lax.optimization_barrier((*arrs, held))
            return out[:-1]

        tail = sent[-1][-1][0]
        for k in range(ep_size - 2):
            for unit, (keep_o, got_o, keep_d, got_d) in enumerate(sent[k]):
                got_o, = after(tail, got_o)
                sent[k][unit] = (keep_o, got_o, keep_d, got_d)
        near = sent[-1][0][0]
        for unit, (keep_o, got_o, keep_d, got_d) in enumerate(sent[-2]):
            got_o, = after(near, got_o)
            if unit:
                got_d, d_gate = lax.optimization_barrier((got_d, d_gate))
            else:
                got_d, = after(near, got_d)
            sent[-2][unit] = (keep_o, got_o, keep_d, got_d)
        sums_far = after(tail, *sums_far)
        for unit in range(2):
            keep_o, got_o, keep_d, got_d = sent[-1][unit]
            got_o, d_gate = lax.optimization_barrier((got_o, d_gate))
            got_d, d_lin = lax.optimization_barrier((got_d, d_lin))
            sent[-1][unit] = (keep_o, got_o, keep_d, got_d)

        def back(k, keep, got):
            total = fold(keep, got)
            return swap(total, k) if k else total

        o_back = [back(k, *sent[k][unit][:2]) for k in range(ep_size) for unit in range(2)]

        tile_rows = (rows >> 1) * 8
        row_first, row_second = tile_rows[:, 0], tile_rows[:, 1]

        half_rows = jax.ShapeDtypeStruct((tok_count, half), jnp.bfloat16)
        o_parts = [arr.reshape(-1, half) for arr in o_back]
        y_half, dn_part = rows_call(
            combine_kernel, tp_vec, [('half', x_loc), ('half', dy_loc), ('row', cols)],
            [half_rows, jax.ShapeDtypeStruct((tok_count, 2), jnp.float32)], tok_count, 512, (o_parts, row_first, row_second))
        dn_part = dn_part.T
        dn_other = swap_tp(dn_part)
        dn = (dn_part + dn_other).T

        def join(own, other):
            whole = jax.ShapeDtypeStruct((tok_count, width), jnp.bfloat16)
            return rows_call(join_kernel, tp_vec, [('row', own), ('row', other)], [whole], tok_count, 1024)[0]

        y_other = swap_tp(y_half)
        y_loc = join(y_half, y_other)
        stats = ((sums_own + sums_far[0]) + sums_far[1]) + sums_far[2]
        frac_first = stats[0, :experts] / tokens
        z_loss = Z_COEF * stats[2, 0] / tokens
        aux_loss = AUX_COEF * experts * jnp.sum(frac_first * stats[1, :experts]) / tokens
        aux_row = (AUX_COEF * experts * frac_first).reshape(1, experts)
        for k in range(ep_size - 2):
            for unit, (keep_o, got_o, keep_d, got_d) in enumerate(sent[k]):
                got_d, = after(y_half, got_d)
                sent[k][unit] = (keep_o, got_o, keep_d, got_d)
        du_back = [back(k, *sent[k][unit][2:]) for k in range(ep_size) for unit in range(2)]
        du_parts = [arr.reshape(-1, half) for arr in du_back]
        dxn, mix, d_scale_half, d_router_half = rows_call(
            norm_kernel, tp_vec,
            [('half', x_loc), ('row', prob), ('row', idx_loc), ('row', dn), ('same', aux_row), ('deep', w_router), ('lanes', scale_row), ('row', cols)],
            [jax.ShapeDtypeStruct((tok_count, half), jnp.float32), jax.ShapeDtypeStruct((tok_count, 1), jnp.float32), jax.ShapeDtypeStruct((1, half), jnp.float32), jax.ShapeDtypeStruct((half, experts), jnp.float32)],
            tok_count, 512, (du_parts, row_first, row_second))
        mix = mix.reshape(tok_count)
        mix = ((mix + swap_tp(mix)) / width).reshape(tok_count, 1)
        dx_half = rows_call(dx_kernel, tp_vec, [('half', x_loc), ('half', dy_loc), ('row', dxn), ('row', cols), ('row', mix)], [half_rows], tok_count, 1024)[0]
        dx_other = swap_tp(dx_half)
        dx_loc = join(dx_half, dx_other)
        d_scale_half = d_scale_half.reshape(half)
        both = jnp.concatenate([d_router_half.reshape(-1), d_scale_half])
        both = lax.dynamic_update_slice_in_dim(jnp.zeros((2, both.shape[0]), jnp.float32), both[None], tp_id, 0)
        both = lax.psum(both, ('tp', 'ep'))
        d_router = both[:, :half * experts].reshape(width, experts)
        d_scale = both[:, half * experts:].reshape(width)
        losses = jnp.stack([z_loss, aux_loss])
        return (y_loc, losses, dx_loc, d_scale, d_router, d_gate, d_lin, d_out)

    tok_spec = P('ep', None)
    in_spec = P('ep', None, 'tp')
    out_spec = P('ep', 'tp', None)
    return jax.shard_map(device_body, mesh=mesh, in_specs=(tok_spec, tok_spec, tok_spec, P(), P(), in_spec, in_spec, out_spec), out_specs=(tok_spec, P(), tok_spec, P(), P(), in_spec, in_spec, out_spec), check_vma=False)
```
